256 devices in a mesh: band: 8 (over z_lo, core), lane: 32 (over z_hi, y, x).
Axes of the slice: x: 4, y: 4, z: 8 (z_hi: 2, z_lo: 4; z = z_hi * 4 + z_lo), core: 2. Of those that a mesh axis runs over, the one named last changes fastest.
Arguments:
- load_terms: float32 [512, 2048, 128], P('band', 'lane'), may hold values from -6 to 6
- start_values: float32 [512, 2048, 128], P('band', 'lane'), may hold values from -6 to 6
- reaction_rate: float32 [512, 2048, 128], P('band', 'lane'), may hold values from 0.1 to 0.9
Outputs:
- solution: float32 [512, 2048, 128], P('band', 'lane')
The draws below stay inside these ranges and needn't reach their ends.
All inputs are finite; a program needn't handle non-finite values.
Results may differ from the reference program's by a relative error of at most 0.0003.
Values sent between devices are 32-bit elements.
No kernel may reach another device: no remote copies, remote signals or barrier semaphores. Data moves between devices by JAX's collectives and lax.ppermute only.
A program may use at most 64 MiB of HBM per device.

```python
import jax
import jax.numpy as jnp
from jax import lax

LAYERS = 128
RATIO = 4
BEFORE = 3
AFTER = 2
INNER = 13
GRID_Y = 512
GRID_X = 2048


def steps_of(stream_key, dims, cuts, smallest, high):
    gain = 1.0
    for position, blocks in cuts:
        steps = jax.random.uniform(jax.random.fold_in(jax.random.fold_in(stream_key, 6), position), (blocks,), jnp.float32, smallest / len(cuts), high / len(cuts))
        gain = gain * jnp.repeat(jnp.exp(steps), dims[position] // blocks).reshape((-1,) + (1,) * (len(dims) - 1 - position))
    return gain


def noise(stream_key, shape, width, limit, cuts=(), dtype=jnp.bfloat16):
    values = jax.random.normal(stream_key, shape, jnp.float32) * width
    if len(cuts) > 0:
        values = steps_of(stream_key, shape, cuts, -0.22, 0.18) * values
    return jnp.clip(values, min=-limit, max=limit).astype(dtype)


def setup_inputs(seed: int = 0) -> dict:
    seeds = jax.random.split(jax.random.key(seed), 4)
    return {
        "load_terms": noise(seeds[0], (GRID_Y, GRID_X, LAYERS), 1.0, 6.0, ((0, 8), (1, 32)), jnp.float32),
        "start_values": noise(seeds[1], (GRID_Y, GRID_X, LAYERS), 1.0, 6.0, ((0, 8), (1, 32)), jnp.float32),
        "reaction_rate": jnp.clip(0.1 + 0.79999997 * jax.random.uniform(seeds[2], (GRID_Y, GRID_X, LAYERS), jnp.float32) ** steps_of(seeds[2], (GRID_Y, GRID_X, LAYERS), ((0, 8), (1, 32)), -0.2, 0.2), 0.1, 0.9),
    }


def cross_sum(padded):
    inner_y, inner_x = padded.shape[0] - 2, padded.shape[1] - 2
    middle_rows = lax.slice_in_dim(padded, 1, 1 + inner_y, axis=0)
    middle_columns = lax.slice_in_dim(padded, 1, 1 + inner_x, axis=1)
    return (lax.slice_in_dim(middle_columns, 0, inner_y, axis=0) + lax.slice_in_dim(middle_columns, 2, 2 + inner_y, axis=0)
            + lax.slice_in_dim(middle_rows, 0, inner_x, axis=1) + lax.slice_in_dim(middle_rows, 2, 2 + inner_x, axis=1))


def smooth_step(padded, values, load, mass_here):
    return values + 0.8 * (load + cross_sum(padded) - (4.0 + mass_here) * values) / (4.0 + mass_here)


def block_means(values):
    cut = values.reshape(values.shape[0] // RATIO, RATIO, values.shape[1] // RATIO, RATIO, values.shape[2])
    return jnp.mean(cut, axis=(1, 3))


def spread_blocks(values):
    return jnp.repeat(jnp.repeat(values, RATIO, axis=0), RATIO, axis=1)


def reference(load_terms, start_values, reaction_rate):
    values = start_values
    for sweep in range(BEFORE):
        values = smooth_step(jnp.pad(values, ((1, 1), (1, 1), (0, 0)), mode="wrap"), values, load_terms, reaction_rate)
    defect = load_terms + cross_sum(jnp.pad(values, ((1, 1), (1, 1), (0, 0)), mode="wrap")) - (4.0 + reaction_rate) * values
    coarse_load, coarse_mass = block_means(defect) * RATIO, block_means(reaction_rate) * RATIO
    coarse_values = jnp.zeros_like(coarse_load)
    for sweep in range(INNER):
        coarse_values = smooth_step(jnp.pad(coarse_values, ((1, 1), (1, 1), (0, 0)), mode="wrap"), coarse_values, coarse_load, coarse_mass)
    values = values + spread_blocks(coarse_values)
    for sweep in range(AFTER):
        values = smooth_step(jnp.pad(values, ((1, 1), (1, 1), (0, 0)), mode="wrap"), values, load_terms, reaction_rate)
    solution = values
    return solution
```

```python
import jax
import jax.numpy as jnp
from jax import lax
from jax.experimental import pallas as pl
from jax.experimental.pallas import tpu as pltpu
from jax.sharding import PartitionSpec as P

RATIO = 4
BEFORE = 3
AFTER = 2
INNER = 13

N = 64
C = N // RATIO
L = 128
DS = BEFORE + AFTER
DF = DS - 1
DEPTH = DS + 2 * DF
R0 = DS
C0 = 8
ROWS = N + 2 * DS
COLS = N + 16
H = INNER
CR = C + 2 * H
CC0 = 16
CCOLS = 48
WIDTHS = [C + 2 * (H + 1 - j) for j in range(1, H + 1)]
STARTS = [sum(WIDTHS[:k]) for k in range(H)]
BANDMSG = -(-sum(WIDTHS) // 8) * 8
FIT = 16 * 2**20

f32 = jnp.float32


def parity(axis):
    return lax.rem(lax.axis_index(axis), 2) == 0


def sds(*shape):
    return jax.ShapeDtypeStruct(shape, f32)


VM = pl.BlockSpec(memory_space=pltpu.VMEM)
ANY = pl.BlockSpec(memory_space=pl.ANY)


def call(body, outs, ins, scratch=(), out_specs=None, aliases=None, flops=10**6, name=None, inner=True):
    return pl.pallas_call(
        body,
        out_shape=[pltpu.VMEM(o.shape, o.dtype) for o in outs] if inner else outs,
        in_specs=ins,
        out_specs=out_specs if out_specs is not None else [VM] * len(outs),
        scratch_shapes=list(scratch),
        input_output_aliases=aliases or {},
        compiler_params=pltpu.CompilerParams(vmem_limit_bytes=FIT),
        cost_estimate=pl.CostEstimate(flops=flops, bytes_accessed=8 * 10**6, transcendentals=0),
        name=name,
    )


def pack_fine(load, start, mass, m_even, m_odd, b_even, b_odd, side, sem_side, sem_band):
    copies = []
    for k, src in enumerate((start, load, mass)):
        for s, at in enumerate((0, N - 8)):
            copies.append(
                pltpu.make_async_copy(src.at[:, pl.ds(at, 8)], side.at[k, s], sem_side.at[k, s])
            )
    even = parity("band")
    bands = []
    for which, (dst, bottom) in enumerate(((b_even, even), (b_odd, jnp.logical_not(even)))):
        at = 0
        for k, (src, depth) in enumerate(((start, DS), (load, DF), (mass, DF))):
            first = jnp.where(bottom, N - depth, 0)
            bands.append(
                pltpu.make_async_copy(
                    src.at[pl.ds(first, depth)], dst.at[pl.ds(at, depth)], sem_band.at[which, k]
                )
            )
            at += depth
    for c in copies:
        c.start()
    for c in bands:
        c.start()
    for c in copies:
        c.wait()

    def pack(dst, s):
        def group(g, carry):
            base = pl.multiple_of(g * (8 * DEPTH), 8)
            for r in range(8):
                at = r * DEPTH
                for k, depth in enumerate((DS, DF, DF)):
                    lo = 0 if s == 0 else 8 - depth
                    dst[pl.ds(base + at, depth), :] = side[k, s, g * 8 + r, lo : lo + depth, :]
                    at += depth
            return carry

        lax.fori_loop(0, N // 8, group, 0)

    lane_even = parity("lane")

    @pl.when(lane_even)
    def _():
        pack(m_even, 1)
        pack(m_odd, 0)

    @pl.when(jnp.logical_not(lane_even))
    def _():
        pack(m_even, 0)
        pack(m_odd, 1)

    for c in bands:
        c.wait()


def pack_corners(m_even, m_odd, c_even, c_odd):
    rows = DF * DEPTH

    def fill(left, right):
        def put(dst, first):
            dst[0:rows, :] = left[first : first + rows, :]
            dst[rows : 2 * rows, :] = right[first : first + rows, :]

        even = parity("band")

        @pl.when(even)
        def _():
            put(c_even, (N - DF) * DEPTH)
            put(c_odd, 0)

        @pl.when(jnp.logical_not(even))
        def _():
            put(c_even, 0)
            put(c_odd, (N - DF) * DEPTH)

    lane_even = parity("lane")

    @pl.when(lane_even)
    def _():
        fill(m_odd, m_even)

    @pl.when(jnp.logical_not(lane_even))
    def _():
        fill(m_even, m_odd)


def pack_coarse_lanes(own, m_even, m_odd):
    def put(right, left):
        for i in range(C):
            row = own(i)
            right[i * H : (i + 1) * H, :] = row[C - H :, :]
            left[i * H : (i + 1) * H, :] = row[:H, :]

    even = parity("lane")

    @pl.when(even)
    def _():
        put(m_even, m_odd)

    @pl.when(jnp.logical_not(even))
    def _():
        put(m_odd, m_even)


def place_coarse_lanes(ext, m_even, m_odd):
    def put(left, right):
        for i in range(C):
            ext[H + i, CC0 - H : CC0, :] = left[i * H : (i + 1) * H, :]
            ext[H + i, CC0 + C : CC0 + C + H, :] = right[i * H : (i + 1) * H, :]

    even = parity("lane")

    @pl.when(even)
    def _():
        put(m_odd, m_even)

    @pl.when(jnp.logical_not(even))
    def _():
        put(m_even, m_odd)


def pack_coarse_bands(ext, b_even, b_odd):
    def put(down, up):
        for j in range(1, H + 1):
            reach, at, wide = H + 1 - j, STARTS[j - 1], WIDTHS[j - 1]
            cols = slice(CC0 - reach, CC0 + C + reach)
            down[at : at + wide, :] = ext[H + C - j, cols, :]
            up[at : at + wide, :] = ext[H + j - 1, cols, :]
        for dst in (down, up):
            dst[sum(WIDTHS) :, :] = jnp.zeros((BANDMSG - sum(WIDTHS), L), f32)

    even = parity("band")

    @pl.when(even)
    def _():
        put(b_even, b_odd)

    @pl.when(jnp.logical_not(even))
    def _():
        put(b_odd, b_even)


def place_coarse_bands(ext, b_even, b_odd):
    def put(above, below):
        for j in range(1, H + 1):
            reach, at, wide = H + 1 - j, STARTS[j - 1], WIDTHS[j - 1]
            cols = slice(CC0 - reach, CC0 + C + reach)
            ext[H - j, cols, :] = above[at : at + wide, :]
            ext[H + C + j - 1, cols, :] = below[at : at + wide, :]

    even = parity("band")

    @pl.when(even)
    def _():
        put(b_odd, b_even)

    @pl.when(jnp.logical_not(even))
    def _():
        put(b_even, b_odd)


def weight(mass):
    return 0.8 / (4.0 + mass)


def sweep_rows(src, dst, w, f, first, last, segments, per=2):
    def one(r):
        for lo, hi in segments:
            around = (
                (src[r - 1, lo:hi, :] + src[r + 1, lo:hi, :])
                + (src[r, lo - 1 : hi - 1, :] + src[r, lo + 1 : hi + 1, :])
                + f[r, lo:hi, :]
            )
            dst[r, lo:hi, :] = 0.2 * src[r, lo:hi, :] + w[r, lo:hi, :] * around

    whole = (last - first) // per

    def group(g, carry):
        for k in range(per):
            one(first + g * per + k)
        return carry

    lax.fori_loop(0, whole, group, 0)
    for r in range(first + whole * per, last):
        one(r)


def gather_columns(line, row):
    line[...] = row
    total = line[pl.ds(0, C, stride=RATIO), :]
    for k in range(1, RATIO):
        total = total + line[pl.ds(k, C, stride=RATIO), :]
    return total * (1.0 / RATIO)


def prepare(load, start, mass, u, f, w, a4, cm, m_even, m_odd, line, sems):
    own = (pl.ds(R0, N), pl.ds(C0, N))
    copies = [
        pltpu.make_async_copy(mass, a4, sems.at[0]),
        pltpu.make_async_copy(load, f.at[own], sems.at[1]),
        pltpu.make_async_copy(start, u.at[own], sems.at[2]),
    ]
    for c in copies:
        c.start()
    copies[0].wait()

    def block(i, carry):
        total = jnp.zeros((N, L), f32)
        for k in range(RATIO):
            r = i * RATIO + k
            m = a4[r]
            total = total + m
            a = 4.0 + m
            a4[r] = a
            w[R0 + r, C0 : C0 + N, :] = 0.8 / a
        cm[i] = gather_columns(line, total)
        return carry

    lax.fori_loop(0, C, block, 0)
    pack_coarse_lanes(lambda i: cm[i], m_even, m_odd)
    for c in copies[1:]:
        c.wait()


FINE_SEGMENTS = ((C0 - DF, C0), (C0, C0 + N), (C0 + N, C0 + N + DF))


def before(u_in, f_in, w_in, a4, cm, re, ro, be, bo, ce, co, mre, mro, v, f, w, mext, l_even, l_odd, mb_even, mb_odd, cl, u, line):
    def rows_copy(g, carry):
        for k in range(2):
            r = R0 + 2 * g + k
            u[r, C0 : C0 + N, :] = u_in[r, C0 : C0 + N, :]
        return carry

    lax.fori_loop(0, N // 2, rows_copy, 0)
    R1, C1 = R0 + N, C0 + N

    def put_left(r, msg, at):
        u[r, C0 - DS : C0, :] = msg[at : at + DS, :]
        f[r, C0 - DF : C0, :] = msg[at + DS : at + DS + DF, :]
        w[r, C0 - DF : C0, :] = weight(msg[at + DS + DF : at + DEPTH, :])

    def put_right(r, msg, at):
        u[r, C1 : C1 + DS, :] = msg[at : at + DS, :]
        f[r, C1 : C1 + DF, :] = msg[at + DS : at + DS + DF, :]
        w[r, C1 : C1 + DF, :] = weight(msg[at + DS + DF : at + DEPTH, :])

    def lanes(left, right):
        def group(g, carry):
            base = pl.multiple_of(g * (8 * DEPTH), 8)
            for r in range(8):
                row, at = R0 + g * 8 + r, base + r * DEPTH
                u[row, C0 - DS : C0, :] = left[pl.ds(at, DS), :]
                f[row, C0 - DF : C0, :] = left[pl.ds(at + DS, DF), :]
                w[row, C0 - DF : C0, :] = weight(left[pl.ds(at + DS + DF, DF), :])
                u[row, C1 : C1 + DS, :] = right[pl.ds(at, DS), :]
                f[row, C1 : C1 + DF, :] = right[pl.ds(at + DS, DF), :]
                w[row, C1 : C1 + DF, :] = weight(right[pl.ds(at + DS + DF, DF), :])
            return carry

        lax.fori_loop(0, N // 8, group, 0)

    lane_even = parity("lane")

    @pl.when(lane_even)
    def _():
        lanes(ro, re)

    @pl.when(jnp.logical_not(lane_even))
    def _():
        lanes(re, ro)

    def bands(above, below, above_c, below_c):
        own = slice(C0, C1)
        for k in range(DS):
            u[k, own, :] = above[k]
            u[R1 + k, own, :] = below[k]
        for k in range(DF):
            f[R0 - DF + k, own, :] = above[DS + k]
            w[R0 - DF + k, own, :] = weight(above[DS + DF + k])
            f[R1 + k, own, :] = below[DS + k]
            w[R1 + k, own, :] = weight(below[DS + DF + k])
            for msg, row in ((above_c, R0 - DF + k), (below_c, R1 + k)):
                put_left(row, msg, k * DEPTH)
                put_right(row, msg, (DF + k) * DEPTH)

    band_even = parity("band")

    @pl.when(band_even)
    def _():
        bands(bo, be, co, ce)

    @pl.when(jnp.logical_not(band_even))
    def _():
        bands(be, bo, ce, co)

    sweep_rows(u, v, w, f, 1, ROWS - 1, FINE_SEGMENTS)
    sweep_rows(v, u, w, f, 2, ROWS - 2, FINE_SEGMENTS)
    sweep_rows(u, v, w, f, 3, ROWS - 3, FINE_SEGMENTS)

    def block(i, carry):
        total = jnp.zeros((N, L), f32)
        for k in range(RATIO):
            q = i * RATIO + k
            r = R0 + q
            total = total + (
                f[r, C0:C1, :]
                + (v[r - 1, C0:C1, :] + v[r + 1, C0:C1, :])
                + (v[r, C0 - 1 : C1 - 1, :] + v[r, C0 + 1 : C1 + 1, :])
                - a4[q] * v[r, C0:C1, :]
            )
        cl[i] = gather_columns(line, total)
        return carry

    lax.fori_loop(0, C, block, 0)
    pack_coarse_lanes(lambda i: cl[i], l_even, l_odd)
    for i in range(C):
        mext[H + i, CC0 : CC0 + C, :] = cm[i]
    place_coarse_lanes(mext, mre, mro)
    pack_coarse_bands(mext, mb_even, mb_odd)


def coarse_bands(cl, re, ro, lext, b_even, b_odd):
    for i in range(C):
        lext[H + i, CC0 : CC0 + C, :] = cl[i]
    place_coarse_lanes(lext, re, ro)
    pack_coarse_bands(lext, b_even, b_odd)


def after(v, f, w, mext_in, lext_in, mbe, mbo, lbe, lbo, out, mext, lext, a, b, wide, t, s):
    span = slice(CC0 - H, CC0 + C + H)
    for i in range(C):
        mext[H + i, span, :] = mext_in[H + i, span, :]
        lext[H + i, span, :] = lext_in[H + i, span, :]
    place_coarse_bands(mext, mbe, mbo)
    place_coarse_bands(lext, lbe, lbo)

    def first(r, carry):
        wc = weight(mext[r, 0:CCOLS, :])
        mext[r, 0:CCOLS, :] = wc
        a[r, 0:CCOLS, :] = wc * lext[r, 0:CCOLS, :]
        return carry

    lax.fori_loop(0, CR, first, 0)
    src, dst = a, b
    for k in range(1, INNER):
        if k <= 4:
            segments = ((4, 8), (8, 40), (40, 44))
        elif k <= 12:
            segments = ((8, 40),)
        sweep_rows(src, dst, mext, lext, k, CR - k, segments)
        src, dst = dst, src
    for i in range(-1, C + 1):
        row = src[H + i, CC0 - 1 : CC0 + C + 1, :]
        for k in range(RATIO):
            wide[pl.ds(k, C + 2, stride=RATIO), :] = row
        for k in range(RATIO):
            q = i * RATIO + k
            if -AFTER <= q < N + AFTER:
                r = R0 + q
                t[r, C0 - 4 : C0 + N + 4, :] = v[r, C0 - 4 : C0 + N + 4, :] + wide[...]
    sweep_rows(t, s, w, f, R0 - 1, R0 + N + 1, ((C0 - 4, C0), (C0, C0 + N), (C0 + N, C0 + N + 4)))

    def last(g, carry):
        for k in range(2):
            q = 2 * g + k
            r = R0 + q
            C1 = C0 + N
            around = (
                (s[r - 1, C0:C1, :] + s[r + 1, C0:C1, :])
                + (s[r, C0 - 1 : C1 - 1, :] + s[r, C0 + 1 : C1 + 1, :])
                + f[r, C0:C1, :]
            )
            out[q] = 0.2 * s[r, C0:C1, :] + w[r, C0:C1, :] * around
        return carry

    lax.fori_loop(0, N // 2, last, 0)


def swap_even(x, axis):
    n = lax.axis_size(axis)
    return lax.ppermute(x, axis, [(i, i ^ 1) for i in range(n)])


def swap_odd(x, axis):
    n = lax.axis_size(axis)
    return lax.ppermute(x, axis, [(i, (i + 1) % n if i % 2 else (i - 1) % n) for i in range(n)])


def shards(load, start, mass):
    dma = pltpu.SemaphoreType.DMA
    lane_msg, band_msg = sds(N * DEPTH, L), sds(DEPTH, N, L)
    me, mo, be, bo = call(
        pack_fine,
        [lane_msg, lane_msg, band_msg, band_msg],
        [ANY] * 3,
        [pltpu.VMEM((3, 2, N, 8, L), f32), dma((3, 2)), dma((2, 3))],
        name="pack_fine",
    )(load, start, mass)
    ro, re = swap_odd(mo, "lane"), swap_even(me, "lane")
    rbo, rbe = swap_odd(bo, "band"), swap_even(be, "band")

    fine = sds(ROWS, COLS, L)
    lane_coarse, band_coarse = sds(C * H, L), sds(BANDMSG, L)
    u, f, w, a4, cm, mme, mmo = call(
        prepare,
        [fine, fine, fine, sds(N, N, L), sds(C, C, L), lane_coarse, lane_coarse],
        [ANY] * 3,
        [pltpu.VMEM((N, L), f32), dma((3,))],
        flops=10**8,
        name="prepare",
    )(load, start, mass)
    rmo, rme = swap_odd(mmo, "lane"), swap_even(mme, "lane")

    corner = sds(2 * DF * DEPTH, L)
    ce, co = call(pack_corners, [corner, corner], [VM] * 2, name="pack_corners")(re, ro)
    rco, rce = swap_odd(co, "band"), swap_even(ce, "band")

    coarse = sds(CR, CCOLS, L)
    v, f, w, mext, le, lo, mbe, mbo, cl = call(
        before,
        [fine, fine, fine, coarse, lane_coarse, lane_coarse, band_coarse, band_coarse, sds(C, C, L)],
        [VM] * 13,
        [pltpu.VMEM((ROWS, COLS, L), f32), pltpu.VMEM((N, L), f32)],
        aliases={1: 1, 2: 2},
        flops=10**8,
        name="before",
    )(u, f, w, a4, cm, re, ro, rbe, rbo, rce, rco, rme, rmo)
    rlo, rle = swap_odd(lo, "lane"), swap_even(le, "lane")
    rmbo, rmbe = swap_odd(mbo, "band"), swap_even(mbe, "band")

    lext, lbe, lbo = call(
        coarse_bands, [coarse, band_coarse, band_coarse], [VM] * 3, name="coarse_bands"
    )(cl, rle, rlo)
    rlbo, rlbe = swap_odd(lbo, "band"), swap_even(lbe, "band")

    coarse_buf = pltpu.VMEM((CR, CCOLS, L), f32)
    fine_buf = pltpu.VMEM((ROWS, COLS, L), f32)
    (out,) = call(
        after,
        [sds(N, N, L)],
        [VM] * 9,
        [coarse_buf] * 4 + [pltpu.VMEM((N + 8, L), f32), fine_buf, fine_buf],
        flops=10**8,
        name="after",
        inner=False,
    )(v, f, w, mext, lext, rmbe, rmbo, rlbe, rlbo)
    return out


def solution(mesh):
    spec = P("band", "lane", None)
    return jax.shard_map(
        shards, mesh=mesh, in_specs=(spec, spec, spec), out_specs=spec, check_vma=False
    )
```

```python
import jax
import jax.numpy as jnp
from jax import lax
from jax.experimental import pallas as pl
from jax.experimental.pallas import tpu as pltpu
from jax.sharding import PartitionSpec as P

RATIO = 4
BEFORE = 3
AFTER = 2
INNER = 13

N = 64
C = N // RATIO
L = 128
DS = BEFORE + AFTER
DF = DS - 1
DEPTH = DS + 2 * DF
R0 = DS
C0 = 8
ROWS = N + 2 * DS
COLS = N + 16
H = INNER
CR = C + 2 * H
CC0 = 16
CCOLS = 48
WIDTHS = [C + 2 * (H + 1 - j) for j in range(1, H + 1)]
STARTS = [sum(WIDTHS[:k]) for k in range(H)]
BANDMSG = -(-sum(WIDTHS) // 8) * 8
FIT = 16 * 2**20

f32 = jnp.float32


def parity(axis):
    return lax.rem(lax.axis_index(axis), 2) == 0


def sds(*shape):
    return jax.ShapeDtypeStruct(shape, f32)


VM = pl.BlockSpec(memory_space=pltpu.VMEM)
HBM = pl.BlockSpec(memory_space=pltpu.HBM)


def call(body, outs, ins, scratch=(), out_specs=None, aliases=None, flops=10**6, name=None, inner=True):
    return pl.pallas_call(
        body,
        out_shape=[pltpu.VMEM(o.shape, o.dtype) for o in outs] if inner else outs,
        in_specs=ins,
        out_specs=out_specs if out_specs is not None else [VM] * len(outs),
        scratch_shapes=list(scratch),
        input_output_aliases=aliases or {},
        compiler_params=pltpu.CompilerParams(vmem_limit_bytes=FIT),
        cost_estimate=pl.CostEstimate(flops=flops, bytes_accessed=8 * 10**6, transcendentals=0),
        name=name,
    )


def pack_fine(load, start, mass_hbm, m_even, m_odd, b_even, b_odd, mass, cm, side, line, sem_side, sem_mass, sem_band):
    whole = pltpu.make_async_copy(mass_hbm, mass, sem_mass.at[0])
    copies = []
    for k, src in enumerate((start, load)):
        for s, at in enumerate((0, N - 8)):
            copies.append(
                pltpu.make_async_copy(src.at[:, pl.ds(at, 8)], side.at[k, s], sem_side.at[k, s])
            )
    even = parity("band")
    bands = []
    for which, (dst, bottom) in enumerate(((b_even, even), (b_odd, jnp.logical_not(even)))):
        at = 0
        for k, (src, depth) in enumerate(((start, DS), (load, DF), (mass_hbm, DF))):
            first = jnp.where(bottom, N - depth, 0)
            bands.append(
                pltpu.make_async_copy(
                    src.at[pl.ds(first, depth)], dst.at[pl.ds(at, depth)], sem_band.at[which, k]
                )
            )
            at += depth
    for c in copies:
        c.start()
    whole.start()
    for c in bands:
        c.start()
    for c in copies:
        c.wait()
    lane_even = parity("lane")

    def pack(dst, s):
        def group(g, carry):
            base = pl.multiple_of(g * (8 * DEPTH), 8)
            for r in range(8):
                at = r * DEPTH
                for k, depth in enumerate((DS, DF)):
                    lo = 0 if s == 0 else 8 - depth
                    dst[pl.ds(base + at, depth), :] = side[k, s, g * 8 + r, lo : lo + depth, :]
                    at += depth
            return carry

        lax.fori_loop(0, N // 8, group, 0)

    @pl.when(lane_even)
    def _():
        pack(m_even, 1)
        pack(m_odd, 0)

    @pl.when(jnp.logical_not(lane_even))
    def _():
        pack(m_even, 0)
        pack(m_odd, 1)

    whole.wait()

    def pack_mass(right, left):
        def group(g, carry):
            base = pl.multiple_of(g * (8 * DEPTH), 8)
            for half in range(2):
                total = None
                for k in range(RATIO):
                    r = half * RATIO + k
                    at = r * DEPTH + DS + DF
                    row = mass[g * 8 + r]
                    total = row if total is None else total + row
                    right[pl.ds(base + at, DF), :] = row[N - DF :, :]
                    left[pl.ds(base + at, DF), :] = row[:DF, :]
                cm[2 * g + half] = gather_columns(line.at[half], total)
            return carry

        lax.fori_loop(0, N // 8, group, 0)
        for i in range(C):
            at = N * DEPTH + i * H
            row = cm[i]
            right[at : at + H, :] = row[C - H :, :]
            left[at : at + H, :] = row[:H, :]

    @pl.when(lane_even)
    def _():
        pack_mass(m_even, m_odd)

    @pl.when(jnp.logical_not(lane_even))
    def _():
        pack_mass(m_odd, m_even)

    for c in bands:
        c.wait()


def pack_corners(m_even, m_odd, c_even, c_odd):
    rows = DF * DEPTH

    def fill(left, right):
        def put(dst, first):
            dst[0:rows, :] = left[first : first + rows, :]
            dst[rows : 2 * rows, :] = right[first : first + rows, :]

        even = parity("band")

        @pl.when(even)
        def _():
            put(c_even, (N - DF) * DEPTH)
            put(c_odd, 0)

        @pl.when(jnp.logical_not(even))
        def _():
            put(c_even, 0)
            put(c_odd, (N - DF) * DEPTH)

    lane_even = parity("lane")

    @pl.when(lane_even)
    def _():
        fill(m_odd, m_even)

    @pl.when(jnp.logical_not(lane_even))
    def _():
        fill(m_even, m_odd)


def pack_coarse_lanes(own, m_even, m_odd):
    def put(right, left):
        for i in range(C):
            row = own(i)
            right[i * H : (i + 1) * H, :] = row[C - H :, :]
            left[i * H : (i + 1) * H, :] = row[:H, :]

    even = parity("lane")

    @pl.when(even)
    def _():
        put(m_even, m_odd)

    @pl.when(jnp.logical_not(even))
    def _():
        put(m_odd, m_even)


def place_coarse_lanes(ext, m_even, m_odd, at=0):
    def put(left, right):
        for i in range(C):
            lo = at + i * H
            ext[H + i, CC0 - H : CC0, :] = left[lo : lo + H, :]
            ext[H + i, CC0 + C : CC0 + C + H, :] = right[lo : lo + H, :]

    even = parity("lane")

    @pl.when(even)
    def _():
        put(m_odd, m_even)

    @pl.when(jnp.logical_not(even))
    def _():
        put(m_even, m_odd)


def pack_coarse_bands(ext, b_even, b_odd):
    def put(down, up):
        for j in range(1, H + 1):
            reach, at, wide = H + 1 - j, STARTS[j - 1], WIDTHS[j - 1]
            cols = slice(CC0 - reach, CC0 + C + reach)
            down[at : at + wide, :] = ext[H + C - j, cols, :]
            up[at : at + wide, :] = ext[H + j - 1, cols, :]
        for dst in (down, up):
            dst[sum(WIDTHS) :, :] = jnp.zeros((BANDMSG - sum(WIDTHS), L), f32)

    even = parity("band")

    @pl.when(even)
    def _():
        put(b_even, b_odd)

    @pl.when(jnp.logical_not(even))
    def _():
        put(b_odd, b_even)


def place_coarse_bands(ext, b_even, b_odd):
    def put(above, below):
        for j in range(1, H + 1):
            reach, at, wide = H + 1 - j, STARTS[j - 1], WIDTHS[j - 1]
            cols = slice(CC0 - reach, CC0 + C + reach)
            ext[H - j, cols, :] = above[at : at + wide, :]
            ext[H + C + j - 1, cols, :] = below[at : at + wide, :]

    even = parity("band")

    @pl.when(even)
    def _():
        put(b_odd, b_even)

    @pl.when(jnp.logical_not(even))
    def _():
        put(b_even, b_odd)


def weight(mass):
    return 0.8 / (4.0 + mass)


def sweep_rows(src, dst, w, f, first, last, segments, per=2):
    def one(r):
        for lo, hi in segments:
            around = (
                (src[r - 1, lo:hi, :] + src[r + 1, lo:hi, :])
                + (src[r, lo - 1 : hi - 1, :] + src[r, lo + 1 : hi + 1, :])
                + f[r, lo:hi, :]
            )
            dst[r, lo:hi, :] = 0.2 * src[r, lo:hi, :] + w[r, lo:hi, :] * around

    whole = (last - first) // per

    def group(g, carry):
        for k in range(per):
            one(first + g * per + k)
        return carry

    lax.fori_loop(0, whole, group, 0)
    for r in range(first + whole * per, last):
        one(r)


def gather_columns(line, row):
    line[...] = row
    total = line[pl.ds(0, C, stride=RATIO), :]
    for k in range(1, RATIO):
        total = total + line[pl.ds(k, C, stride=RATIO), :]
    return total * (1.0 / RATIO)


def prepare(load, start, mass, u, f, w, a4, sems):
    own = (pl.ds(R0, N), pl.ds(C0, N))
    copies = [
        pltpu.make_async_copy(load, f.at[own], sems.at[0]),
        pltpu.make_async_copy(start, u.at[own], sems.at[1]),
    ]
    for c in copies:
        c.start()

    def group(g, carry):
        for k in range(2):
            r = g * 2 + k
            a = 4.0 + mass[r]
            a4[r] = a
            w[R0 + r, C0 : C0 + N, :] = 0.8 / a
        return carry

    lax.fori_loop(0, N // 2, group, 0)
    for c in copies:
        c.wait()


FINE_SEGMENTS = ((C0 - DF, C0), (C0, C0 + N), (C0 + N, C0 + N + DF))


def before(u_in, f_in, w_in, a4, cm, re, ro, be, bo, ce, co, v, f, w, mext, l_even, l_odd, mb_even, mb_odd, cl, u, line):
    def rows_copy(g, carry):
        for k in range(2):
            r = R0 + 2 * g + k
            u[r, C0 : C0 + N, :] = u_in[r, C0 : C0 + N, :]
        return carry

    lax.fori_loop(0, N // 2, rows_copy, 0)
    R1, C1 = R0 + N, C0 + N

    def put_left(r, msg, at):
        u[r, C0 - DS : C0, :] = msg[at : at + DS, :]
        f[r, C0 - DF : C0, :] = msg[at + DS : at + DS + DF, :]
        w[r, C0 - DF : C0, :] = weight(msg[at + DS + DF : at + DEPTH, :])

    def put_right(r, msg, at):
        u[r, C1 : C1 + DS, :] = msg[at : at + DS, :]
        f[r, C1 : C1 + DF, :] = msg[at + DS : at + DS + DF, :]
        w[r, C1 : C1 + DF, :] = weight(msg[at + DS + DF : at + DEPTH, :])

    def lanes(left, right):
        def group(g, carry):
            base = pl.multiple_of(g * (8 * DEPTH), 8)
            for r in range(8):
                row, at = R0 + g * 8 + r, base + r * DEPTH
                u[row, C0 - DS : C0, :] = left[pl.ds(at, DS), :]
                f[row, C0 - DF : C0, :] = left[pl.ds(at + DS, DF), :]
                w[row, C0 - DF : C0, :] = weight(left[pl.ds(at + DS + DF, DF), :])
                u[row, C1 : C1 + DS, :] = right[pl.ds(at, DS), :]
                f[row, C1 : C1 + DF, :] = right[pl.ds(at + DS, DF), :]
                w[row, C1 : C1 + DF, :] = weight(right[pl.ds(at + DS + DF, DF), :])
            return carry

        lax.fori_loop(0, N // 8, group, 0)

    lane_even = parity("lane")

    @pl.when(lane_even)
    def _():
        lanes(ro, re)

    @pl.when(jnp.logical_not(lane_even))
    def _():
        lanes(re, ro)

    def bands(above, below, above_c, below_c):
        own = slice(C0, C1)
        for k in range(DS):
            u[k, own, :] = above[k]
            u[R1 + k, own, :] = below[k]
        for k in range(DF):
            f[R0 - DF + k, own, :] = above[DS + k]
            w[R0 - DF + k, own, :] = weight(above[DS + DF + k])
            f[R1 + k, own, :] = below[DS + k]
            w[R1 + k, own, :] = weight(below[DS + DF + k])
            for msg, row in ((above_c, R0 - DF + k), (below_c, R1 + k)):
                put_left(row, msg, k * DEPTH)
                put_right(row, msg, (DF + k) * DEPTH)

    band_even = parity("band")

    @pl.when(band_even)
    def _():
        bands(bo, be, co, ce)

    @pl.when(jnp.logical_not(band_even))
    def _():
        bands(be, bo, ce, co)

    sweep_rows(u, v, w, f, 1, ROWS - 1, FINE_SEGMENTS)
    sweep_rows(v, u, w, f, 2, ROWS - 2, FINE_SEGMENTS)
    sweep_rows(u, v, w, f, 3, ROWS - 3, FINE_SEGMENTS)

    def block(i, carry):
        total = jnp.zeros((N, L), f32)
        for k in range(RATIO):
            q = i * RATIO + k
            r = R0 + q
            total = total + (
                f[r, C0:C1, :]
                + (v[r - 1, C0:C1, :] + v[r + 1, C0:C1, :])
                + (v[r, C0 - 1 : C1 - 1, :] + v[r, C0 + 1 : C1 + 1, :])
                - a4[q] * v[r, C0:C1, :]
            )
        cl[i] = gather_columns(line, total)
        return carry

    lax.fori_loop(0, C, block, 0)
    pack_coarse_lanes(lambda i: cl[i], l_even, l_odd)
    for i in range(C):
        mext[H + i, CC0 : CC0 + C, :] = cm[i]
    place_coarse_lanes(mext, re, ro, N * DEPTH)
    pack_coarse_bands(mext, mb_even, mb_odd)


def coarse_bands(cl, re, ro, lext, b_even, b_odd):
    for i in range(C):
        lext[H + i, CC0 : CC0 + C, :] = cl[i]
    place_coarse_lanes(lext, re, ro)
    pack_coarse_bands(lext, b_even, b_odd)


def coarse_weights(mext, mbe, mbo, wext, ext):
    span = slice(CC0 - H, CC0 + C + H)
    for i in range(C):
        ext[H + i, span, :] = mext[H + i, span, :]
    place_coarse_bands(ext, mbe, mbo)

    def group(g, carry):
        for k in range(2):
            r = g * 2 + k
            wext[r] = weight(ext[r])
        return carry

    lax.fori_loop(0, CR // 2, group, 0)


def after(v, f, w, mext, lext_in, lbe, lbo, out, lext, a, b, wide, t, s):
    span = slice(CC0 - H, CC0 + C + H)
    for i in range(C):
        lext[H + i, span, :] = lext_in[H + i, span, :]
    place_coarse_bands(lext, lbe, lbo)

    def first(r, carry):
        a[r] = mext[r] * lext[r]
        return carry

    lax.fori_loop(0, CR, first, 0)
    src, dst = a, b
    for k in range(1, INNER):
        if k <= 4:
            segments = ((4, 8), (8, 40), (40, 44))
        elif k <= 12:
            segments = ((8, 40),)
        sweep_rows(src, dst, mext, lext, k, CR - k, segments)
        src, dst = dst, src
    for i in range(-1, C + 1):
        row = src[H + i, CC0 - 1 : CC0 + C + 1, :]
        for k in range(RATIO):
            wide[pl.ds(k, C + 2, stride=RATIO), :] = row
        for k in range(RATIO):
            q = i * RATIO + k
            if -AFTER <= q < N + AFTER:
                r = R0 + q
                t[r, C0 - 4 : C0 + N + 4, :] = v[r, C0 - 4 : C0 + N + 4, :] + wide[...]
    sweep_rows(t, s, w, f, R0 - 1, R0 + N + 1, ((C0 - 4, C0), (C0, C0 + N), (C0 + N, C0 + N + 4)))

    def last(g, carry):
        for k in range(2):
            q = 2 * g + k
            r = R0 + q
            C1 = C0 + N
            around = (
                (s[r - 1, C0:C1, :] + s[r + 1, C0:C1, :])
                + (s[r, C0 - 1 : C1 - 1, :] + s[r, C0 + 1 : C1 + 1, :])
                + f[r, C0:C1, :]
            )
            out[q] = 0.2 * s[r, C0:C1, :] + w[r, C0:C1, :] * around
        return carry

    lax.fori_loop(0, N // 2, last, 0)


def swap_even(x, axis):
    n = lax.axis_size(axis)
    return lax.ppermute(x, axis, [(i, i ^ 1) for i in range(n)])


def swap_odd(x, axis):
    n = lax.axis_size(axis)
    return lax.ppermute(x, axis, [(i, (i + 1) % n if i % 2 else (i - 1) % n) for i in range(n)])


def shards(load, start, mass):
    load, start, mass = (pltpu.with_memory_space_constraint(x, pltpu.HBM) for x in (load, start, mass))
    dma = pltpu.SemaphoreType.DMA
    own, fine, corner = sds(N, N, L), sds(ROWS, COLS, L), sds(2 * DF * DEPTH, L)
    lane_msg, band_msg = sds(N * DEPTH + C * H, L), sds(DEPTH, N, L)
    lane_coarse, band_coarse = sds(C * H, L), sds(BANDMSG, L)
    coarse, own_coarse = sds(CR, CCOLS, L), sds(C, C, L)
    coarse_buf, fine_buf = pltpu.VMEM((CR, CCOLS, L), f32), pltpu.VMEM((ROWS, COLS, L), f32)

    me, mo, be, bo, mass_in, cm = call(
        pack_fine,
        [lane_msg, lane_msg, band_msg, band_msg, own, own_coarse],
        [HBM] * 3,
        [pltpu.VMEM((2, 2, N, 8, L), f32), pltpu.VMEM((2, N, L), f32), dma((2, 2)), dma((1,)), dma((2, 3))],
        name="pack_fine",
    )(load, start, mass)
    ro, re = swap_odd(mo, "lane"), swap_even(me, "lane")
    rbo, rbe = swap_odd(bo, "band"), swap_even(be, "band")

    u, f, w, a4 = call(
        prepare,
        [fine, fine, fine, own],
        [HBM, HBM, VM],
        [dma((2,))],
        flops=10**8,
        name="prepare",
    )(load, start, mass_in)

    ce, co = call(pack_corners, [corner, corner], [VM] * 2, name="pack_corners")(re, ro)
    rco, rce = swap_odd(co, "band"), swap_even(ce, "band")

    v, f, w, mext, le, lo, mbe, mbo, cl = call(
        before,
        [fine, fine, fine, coarse, lane_coarse, lane_coarse, band_coarse, band_coarse, own_coarse],
        [VM] * 11,
        [fine_buf, pltpu.VMEM((N, L), f32)],
        aliases={1: 1, 2: 2},
        flops=10**8,
        name="before",
    )(u, f, w, a4, cm, re, ro, rbe, rbo, rce, rco)
    rlo, rle = swap_odd(lo, "lane"), swap_even(le, "lane")
    rmbo, rmbe = swap_odd(mbo, "band"), swap_even(mbe, "band")

    lext, lbe, lbo = call(
        coarse_bands, [coarse, band_coarse, band_coarse], [VM] * 3, name="coarse_bands"
    )(cl, rle, rlo)
    rlbo, rlbe = swap_odd(lbo, "band"), swap_even(lbe, "band")
    (wext,) = call(
        coarse_weights, [coarse], [VM] * 3, [coarse_buf], flops=10**7, name="coarse_weights"
    )(mext, rmbe, rmbo)

    (out,) = call(
        after,
        [own],
        [VM] * 7,
        [coarse_buf] * 3 + [pltpu.VMEM((N + 8, L), f32), fine_buf, fine_buf],
        flops=10**8,
        name="after",
        inner=False,
    )(v, f, w, wext, lext, rlbe, rlbo)
    return out


def solution(mesh):
    spec = P("band", "lane", None)
    return jax.shard_map(
        shards, mesh=mesh, in_specs=(spec, spec, spec), out_specs=spec, check_vma=False
    )
```

```python
import jax
import jax.numpy as jnp
from jax import lax
from jax.experimental import pallas as pl
from jax.experimental.pallas import tpu as pltpu
from jax.sharding import PartitionSpec as P

RATIO = 4
BEFORE = 3
AFTER = 2
INNER = 13

N = 64
C = N // RATIO
L = 128
DS = BEFORE + 1
DF = DS - 1
DEPTH = DS + 2 * DF
AT_LOAD, AT_MASS = N * DS, N * (DS + DF)
FINE = N * DEPTH
R0, C0 = DS, 12
R1, C1 = R0 + N, C0 + N
ROWS, COLS = R1 + DS, C1 + 12
LEFT, RIGHT = slice(C0 - 4, C0 + 4), slice(C1 - 4, C1 + 4)
FULL = ((C0 - 4, C0 + 20), (C0 + 20, C0 + 44), (C0 + 44, C0 + 68))
EDGES = ((C0 - 4, C0 + 4), (C1 - 4, C1 + 4))
H = INNER
CR0, CC0 = H, 20
CR, CCOLS = C + 2 * H, 56
WIDTHS = [C + 2 * (H + 1 - j) for j in range(1, H + 1)]
STARTS = [sum(WIDTHS[:k]) for k in range(H)]
BAND_COARSE = -(-sum(WIDTHS) // 8) * 8
BAND_RIM = N + 8
LANE_COARSE = C * H
FIT = 16 * 2**20

f32 = jnp.float32


def parity(axis):
    return lax.rem(lax.axis_index(axis), 2) == 0


def either(test, one, other):
    @pl.when(test)
    def _():
        one()

    @pl.when(jnp.logical_not(test))
    def _():
        other()


def sds(*shape):
    return jax.ShapeDtypeStruct(shape, f32)


VM = pl.BlockSpec(memory_space=pltpu.VMEM)
HBM = pl.BlockSpec(memory_space=pltpu.HBM)


def call(body, outs, ins, scratch=(), aliases=None, flops=10**6, name=None, inner=True):
    return pl.pallas_call(
        body,
        out_shape=[pltpu.VMEM(o.shape, o.dtype) for o in outs] if inner else outs,
        in_specs=ins,
        out_specs=[VM] * len(outs),
        scratch_shapes=list(scratch),
        input_output_aliases=aliases or {},
        compiler_params=pltpu.CompilerParams(vmem_limit_bytes=FIT),
        cost_estimate=pl.CostEstimate(flops=flops, bytes_accessed=8 * 10**6, transcendentals=0),
        name=name,
    )


def loop(count, per, body):
    def turn(g, carry):
        for k in range(per):
            body(g * per + k)
        return carry

    lax.fori_loop(0, count // per, turn, 0)


def gather_columns(line, row):
    line[...] = row
    total = line[pl.ds(0, C, stride=RATIO), :]
    for k in range(1, RATIO):
        total = total + line[pl.ds(k, C, stride=RATIO), :]
    return total * (1.0 / RATIO)


def pack_fine(load, start, mass_hbm, m_even, m_odd, b_even, b_odd, mass, cm, side, line, sem_side, sem_mass, sem_band):
    whole = pltpu.make_async_copy(mass_hbm, mass, sem_mass.at[0])
    copies = []
    for k, src in enumerate((start, load)):
        for s, at in enumerate((0, N - 8)):
            copies.append(
                pltpu.make_async_copy(src.at[:, pl.ds(at, 8)], side.at[k, s], sem_side.at[k, s])
            )
    even = parity("band")
    bands = []
    for which, (dst, bottom) in enumerate(((b_even, even), (b_odd, jnp.logical_not(even)))):
        at = 0
        for k, (src, depth) in enumerate(((start, DS), (load, DF), (mass_hbm, DF))):
            first = jnp.where(bottom, N - depth, 0)
            bands.append(
                pltpu.make_async_copy(
                    src.at[pl.ds(first, depth)], dst.at[pl.ds(at, depth)], sem_band.at[which, k]
                )
            )
            at += depth
    for c in copies:
        c.start()
    whole.start()
    for c in bands:
        c.start()
    for c in copies:
        c.wait()

    def pack(right, left):
        def group(g, carry):
            for k, (depth, field) in enumerate(((DS, 0), (DF, AT_LOAD))):
                base = pl.multiple_of(g * (8 * depth), 8)
                for r in range(8):
                    at = field + base + r * depth
                    right[pl.ds(at, depth), :] = side[k, 1, g * 8 + r, 8 - depth :, :]
                    left[pl.ds(at, depth), :] = side[k, 0, g * 8 + r, :depth, :]
            return carry

        lax.fori_loop(0, N // 8, group, 0)

    lane_even = parity("lane")
    either(lane_even, lambda: pack(m_even, m_odd), lambda: pack(m_odd, m_even))
    whole.wait()

    def pack_mass(right, left):
        def group(g, carry):
            base = pl.multiple_of(g * (8 * DF), 8)
            for half in range(2):
                total = None
                for k in range(RATIO):
                    r = half * RATIO + k
                    at = AT_MASS + base + r * DF
                    row = mass[g * 8 + r]
                    total = row if total is None else total + row
                    right[pl.ds(at, DF), :] = row[N - DF :, :]
                    left[pl.ds(at, DF), :] = row[:DF, :]
                cm[2 * g + half] = gather_columns(line.at[half], total)
            return carry

        lax.fori_loop(0, N // 8, group, 0)
        pack_coarse_lanes(cm, right, left, FINE)

    either(lane_even, lambda: pack_mass(m_even, m_odd), lambda: pack_mass(m_odd, m_even))
    for c in bands:
        c.wait()


def pack_corners(m_even, m_odd, token, c_even, c_odd):
    del token

    def fill(left, right):
        def put(dst, bottom):
            at = 0
            for src in (left, right):
                for field, depth in ((0, DS), (AT_LOAD, DF), (AT_MASS, DF)):
                    lo, size = field + (N - DF) * depth * bottom, DF * depth
                    dst[at : at + size, :] = src[lo : lo + size, :]
                    at += size

        either(
            parity("band"),
            lambda: (put(c_even, 1), put(c_odd, 0)),
            lambda: (put(c_even, 0), put(c_odd, 1)),
        )

    either(parity("lane"), lambda: fill(m_odd, m_even), lambda: fill(m_even, m_odd))


def pack_coarse_lanes(own, right, left, at):
    for i in range(C):
        lo = at + i * H
        row = own[i]
        right[lo : lo + H, :] = row[C - H :, :]
        left[lo : lo + H, :] = row[:H, :]


def place_coarse_lanes(ext, left, right, at):
    for i in range(C):
        lo = at + i * H
        ext[CR0 + i, CC0 - H : CC0, :] = left[lo : lo + H, :]
        ext[CR0 + i, CC0 + C : CC0 + C + H, :] = right[lo : lo + H, :]


def pack_coarse_bands(ext, down, up):
    for j in range(1, H + 1):
        reach, at, wide = H + 1 - j, STARTS[j - 1], WIDTHS[j - 1]
        cols = slice(CC0 - reach, CC0 + C + reach)
        down[at : at + wide, :] = ext[CR0 + C - j, cols, :]
        up[at : at + wide, :] = ext[CR0 + j - 1, cols, :]
    for dst in (down, up):
        dst[sum(WIDTHS) : BAND_COARSE, :] = jnp.zeros((BAND_COARSE - sum(WIDTHS), L), f32)


def place_coarse_bands(ext, above, below):
    for j in range(1, H + 1):
        reach, at, wide = H + 1 - j, STARTS[j - 1], WIDTHS[j - 1]
        cols = slice(CC0 - reach, CC0 + C + reach)
        ext[CR0 - j, cols, :] = above[at : at + wide, :]
        ext[CR0 + C + j - 1, cols, :] = below[at : at + wide, :]


def weight(mass):
    return 0.8 / (4.0 + mass)


def sweep_rows(src, dst, w, f, first, last, segments, per=4):
    def some(r, count):
        for lo, hi in segments:
            line = [src[r - 1 + k, lo:hi, :] for k in range(count + 2)]
            for k in range(count):
                q = r + k
                around = (line[k] + line[k + 2]) + (
                    src[q, lo - 1 : hi - 1, :] + src[q, lo + 1 : hi + 1, :]
                )
                dst[q, lo:hi, :] = 0.2 * line[k + 1] + w[q, lo:hi, :] * (f[q, lo:hi, :] + around)

    whole = (last - first) // per
    if whole > 1:

        def group(g, carry):
            some(first + g * per, per)
            return carry

        lax.fori_loop(0, whole, group, 0)
        first = first + whole * per
    for r in range(first, last, per):
        some(r, min(per, last - r))


def defect_sum(v, f, a4, first, lo, hi):
    total = None
    line = [v[first - 1 + k, lo:hi, :] for k in range(RATIO + 2)]
    for k in range(RATIO):
        q = first + k
        around = (line[k] + line[k + 2]) + (v[q, lo - 1 : hi - 1, :] + v[q, lo + 1 : hi + 1, :])
        one = (f[q, lo:hi, :] + around) - a4[q, lo:hi, :] * line[k + 1]
        total = one if total is None else total + one
    return total


def prepare(load, start, mass, u, f, w, a4, v1, v2, v3, cl, token, load_in, start_in, line, sems):
    copies = [
        pltpu.make_async_copy(load, load_in, sems.at[0]),
        pltpu.make_async_copy(start, start_in, sems.at[1]),
    ]
    for c in copies:
        c.start()

    def weights(r):
        a = 4.0 + mass[r]
        a4[R0 + r, C0:C1, :] = a
        w[R0 + r, C0:C1, :] = 0.8 / a

    loop(N, 2, weights)
    for c in copies:
        c.wait()

    def place(r):
        f[R0 + r, C0:C1, :] = load_in[r]
        u[R0 + r, C0:C1, :] = start_in[r]

    loop(N, 2, place)
    sweep_rows(u, v1, w, f, R0 + 1, R1 - 1, FULL)
    sweep_rows(v1, v2, w, f, R0 + 2, R1 - 2, FULL)
    sweep_rows(v2, v3, w, f, R0 + 3, R1 - 3, FULL)

    def block(i, carry):
        cl[i] = gather_columns(line, defect_sum(v3, f, a4, R0 + RATIO * i, C0, C1))
        return carry

    lax.fori_loop(1, C - 1, block, 0)
    token[...] = jnp.zeros((8, L), f32)


def before(u_in, f_in, w_in, v1_in, v2_in, v3_in, cl_in, a4, cm, re, ro, be, bo, ce, co, u, f, w, v1, v2, v3, cl, mext, l_even, l_odd, mb_even, mb_odd, wl, wr, wc, line):
    del u_in, f_in, w_in, v1_in, v2_in, v3_in, cl_in

    def lanes(left, right):
        for msg, out in ((left, wl), (right, wr)):
            out[...] = weight(msg[AT_MASS:FINE, :])
        for msg, out, cs, cf in ((left, wl, C0 - DS, C0 - DF), (right, wr, C1, C1)):

            def group(g, carry):
                s0, f0 = pl.multiple_of(g * (8 * DS), 8), pl.multiple_of(g * (8 * DF), 8)
                for r in range(8):
                    row = R0 + g * 8 + r
                    u[row, cs : cs + DS, :] = msg[pl.ds(s0 + r * DS, DS), :]
                    f[row, cf : cf + DF, :] = msg[pl.ds(AT_LOAD + f0 + r * DF, DF), :]
                    w[row, cf : cf + DF, :] = out[pl.ds(f0 + r * DF, DF), :]
                return carry

            lax.fori_loop(0, N // 8, group, 0)
        for i in range(C):
            mext[CR0 + i, CC0 : CC0 + C, :] = cm[i]
        place_coarse_lanes(mext, left, right, FINE)

    lane_even, band_even = parity("lane"), parity("band")
    either(lane_even, lambda: lanes(ro, re), lambda: lanes(re, ro))

    def bands(above, below, above_c, below_c):
        own = slice(C0, C1)
        for msg, row in ((above, R0), (below, R1)):
            first = row - DS if row == R0 else row
            for k in range(DS):
                u[first + k, own, :] = msg[k]
            first = row - DF if row == R0 else row
            for k in range(DF):
                f[first + k, own, :] = msg[DS + k]
                w[first + k, own, :] = weight(msg[DS + DF + k])
        for msg, first in ((above_c, R0 - DF), (below_c, R1)):
            half = DF * DEPTH
            wc[...] = weight(msg[...])
            for at, cs, cf in ((0, C0 - DS, C0 - DF), (half, C1, C1)):
                for k in range(DF):
                    row = first + k
                    s0, l0, m0 = at + k * DS, at + DF * DS + k * DF, at + DF * (DS + DF) + k * DF
                    u[row, cs : cs + DS, :] = msg[s0 : s0 + DS, :]
                    f[row, cf : cf + DF, :] = msg[l0 : l0 + DF, :]
                    w[row, cf : cf + DF, :] = wc[m0 : m0 + DF, :]

    either(band_even, lambda: bands(bo, be, co, ce), lambda: bands(be, bo, ce, co))

    for src, dst, k in ((u, v1, 1), (v1, v2, 2), (v2, v3, 3)):
        reach = BEFORE + 1 - k
        sweep_rows(src, dst, w, f, R0 - reach, R0 + k, FULL)
        sweep_rows(src, dst, w, f, R1 - k, R1 + reach, FULL)
        sweep_rows(src, dst, w, f, R0 + k, R1 - k, EDGES)

    for i in (0, C - 1):
        cl[i] = gather_columns(line, defect_sum(v3, f, a4, R0 + RATIO * i, C0, C1))

    def rims(i, carry):
        row = R0 + RATIO * i
        left = defect_sum(v3, f, a4, row, C0 - 4, C0 + 4)
        right = defect_sum(v3, f, a4, row, C1 - 4, C1 + 4)
        cl[i, 0:1, :] = jnp.sum(left[4:8, :], axis=0, keepdims=True) * (1.0 / RATIO)
        cl[i, C - 1 : C, :] = jnp.sum(right[0:4, :], axis=0, keepdims=True) * (1.0 / RATIO)
        return carry

    lax.fori_loop(1, C - 1, rims, 0)

    def out_lanes(right, left):
        pack_coarse_lanes(cl, right, left, 0)

        def group(g, carry):
            base = pl.multiple_of(g * 8, 8)
            for r in range(8):
                row = R0 + g * 8 + r
                right[pl.ds(LANE_COARSE + base + r, 1), :] = v3[row, C1 - 2 : C1 - 1, :]
                left[pl.ds(LANE_COARSE + base + r, 1), :] = v3[row, C0 + 1 : C0 + 2, :]
            return carry

        lax.fori_loop(0, N // 8, group, 0)

    either(lane_even, lambda: out_lanes(l_even, l_odd), lambda: out_lanes(l_odd, l_even))

    def out_bands(down, up):
        pack_coarse_bands(mext, down, up)
        for dst, rim, edge in ((down, R1 - 2, R1 - 1), (up, R0 + 1, R0)):
            at = BAND_COARSE
            dst[at : at + N, :] = v3[rim, C0:C1, :]
            dst[at + N : at + N + 8, :] = jnp.zeros((8, L), f32)
            dst[at + N : at + N + 1, :] = v3[edge, C0 - 1 : C0, :]
            dst[at + N + 1 : at + N + 2, :] = v3[edge, C1 : C1 + 1, :]

    either(band_even, lambda: out_bands(mb_even, mb_odd), lambda: out_bands(mb_odd, mb_even))


def coarse_bands(cl, re, ro, lext, b_even, b_odd):
    for i in range(C):
        lext[CR0 + i, CC0 : CC0 + C, :] = cl[i]
    either(
        parity("lane"),
        lambda: place_coarse_lanes(lext, ro, re, 0),
        lambda: place_coarse_lanes(lext, re, ro, 0),
    )
    either(
        parity("band"),
        lambda: pack_coarse_bands(lext, b_even, b_odd),
        lambda: pack_coarse_bands(lext, b_odd, b_even),
    )


def between(v_in, mext, mbe, mbo, le, lo, v, wext, ext):
    del v_in

    def lanes(left, right):
        def group(g, carry):
            base = pl.multiple_of(g * 8, 8)
            for r in range(8):
                row = R0 + g * 8 + r
                v[row, C0 - 2 : C0 - 1, :] = left[pl.ds(LANE_COARSE + base + r, 1), :]
                v[row, C1 + 1 : C1 + 2, :] = right[pl.ds(LANE_COARSE + base + r, 1), :]
            return carry

        lax.fori_loop(0, N // 8, group, 0)

    either(parity("lane"), lambda: lanes(lo, le), lambda: lanes(le, lo))
    span = slice(CC0 - H, CC0 + C + H)
    for i in range(C):
        ext[CR0 + i, span, :] = mext[CR0 + i, span, :]

    def bands(above, below):
        place_coarse_bands(ext, above, below)
        for msg, rim, edge in ((above, R0 - 2, R0 - 1), (below, R1 + 1, R1)):
            at = BAND_COARSE
            v[rim, C0:C1, :] = msg[at : at + N, :]
            v[edge, C0 - 1 : C0, :] = msg[at + N : at + N + 1, :]
            v[edge, C1 : C1 + 1, :] = msg[at + N + 1 : at + N + 2, :]

    either(parity("band"), lambda: bands(mbo, mbe), lambda: bands(mbe, mbo))

    def weights(r):
        wext[r] = weight(ext[r])

    loop(CR, 2, weights)


def after(v, f, w, wext, lext_in, lbe, lbo, out, lext, a, b, wide, t, s):
    span = slice(CC0 - H, CC0 + C + H)
    for i in range(C):
        lext[CR0 + i, span, :] = lext_in[CR0 + i, span, :]
    either(
        parity("band"),
        lambda: place_coarse_bands(lext, lbo, lbe),
        lambda: place_coarse_bands(lext, lbe, lbo),
    )

    def first(r):
        a[r] = wext[r] * lext[r]

    loop(CR, 2, first)
    src, dst = a, b
    for k in range(1, INNER):
        segments = ((8, 24), (24, 48)) if k <= 8 else ((16, 40),)
        sweep_rows(src, dst, wext, lext, k, CR - k, segments)
        src, dst = dst, src
    for i in range(-1, C + 1):
        row = src[CR0 + i, CC0 - 1 : CC0 + C + 1, :]
        for k in range(RATIO):
            wide[pl.ds(k, C + 2, stride=RATIO), :] = row
        for k in range(RATIO):
            q = i * RATIO + k
            if -AFTER <= q < N + AFTER:
                t[R0 + q, C0 - 4 : C1 + 4, :] = v[R0 + q, C0 - 4 : C1 + 4, :] + wide[...]
    sweep_rows(t, s, w, f, R0 - 1, R1 + 1, FULL, per=2)

    def last(r, carry):
        for lo, hi in ((0, 32), (32, 64)):
            line = [s[R0 + 4 * r - 1 + k, C0 + lo : C0 + hi, :] for k in range(6)]
            for k in range(4):
                q = R0 + 4 * r + k
                around = (line[k] + line[k + 2]) + (
                    s[q, C0 + lo - 1 : C0 + hi - 1, :] + s[q, C0 + lo + 1 : C0 + hi + 1, :]
                )
                out[4 * r + k, lo:hi, :] = 0.2 * line[k + 1] + w[q, C0 + lo : C0 + hi, :] * (
                    f[q, C0 + lo : C0 + hi, :] + around
                )
        return carry

    lax.fori_loop(0, N // 4, last, 0)


def swap_even(x, axis):
    n = lax.axis_size(axis)
    return lax.ppermute(x, axis, [(i, i ^ 1) for i in range(n)])


def swap_odd(x, axis):
    n = lax.axis_size(axis)
    return lax.ppermute(x, axis, [(i, (i + 1) % n if i % 2 else (i - 1) % n) for i in range(n)])


def shards(load, start, mass):
    load, start, mass = (pltpu.with_memory_space_constraint(x, pltpu.HBM) for x in (load, start, mass))
    dma = pltpu.SemaphoreType.DMA
    own, fine = sds(N, N, L), sds(ROWS, COLS, L)
    corner = sds(2 * DF * DEPTH, L)
    lane_msg, band_msg = sds(FINE + LANE_COARSE, L), sds(DEPTH, N, L)
    lane_coarse, band_coarse = sds(LANE_COARSE + N, L), sds(BAND_COARSE, L)
    band_both = sds(BAND_COARSE + BAND_RIM, L)
    coarse, own_coarse = sds(CR, CCOLS, L), sds(C, C, L)
    coarse_buf, fine_buf = pltpu.VMEM((CR, CCOLS, L), f32), pltpu.VMEM((ROWS, COLS, L), f32)
    own_buf, line = pltpu.VMEM((N, N, L), f32), pltpu.VMEM((N, L), f32)

    me, mo, be, bo, mass_in, cm = call(
        pack_fine,
        [lane_msg, lane_msg, band_msg, band_msg, own, own_coarse],
        [HBM] * 3,
        [pltpu.VMEM((2, 2, N, 8, L), f32), pltpu.VMEM((2, N, L), f32), dma((2, 2)), dma((1,)), dma((2, 3))],
        name="pack_fine",
    )(load, start, mass)
    ro, re = swap_odd(mo, "lane"), swap_even(me, "lane")
    rbo, rbe = swap_odd(bo, "band"), swap_even(be, "band")

    u, f, w, a4, v1, v2, v3, cl, token = call(
        prepare,
        [fine] * 7 + [own_coarse, sds(8, L)],
        [HBM, HBM, VM],
        [own_buf, own_buf, line, dma((2,))],
        flops=10**8,
        name="prepare",
    )(load, start, mass_in)

    ce, co = call(pack_corners, [corner, corner], [VM] * 3, name="pack_corners")(re, ro, token)
    rco, rce = swap_odd(co, "band"), swap_even(ce, "band")

    u, f, w, v1, v2, v3, cl, mext, le, lo, mbe, mbo = call(
        before,
        [fine] * 6 + [own_coarse, coarse, lane_coarse, lane_coarse, band_both, band_both],
        [VM] * 15,
        [pltpu.VMEM((N * DF, L), f32), pltpu.VMEM((N * DF, L), f32), pltpu.VMEM(corner.shape, f32), line],
        aliases={k: k for k in range(7)},
        flops=10**8,
        name="before",
    )(u, f, w, v1, v2, v3, cl, a4, cm, re, ro, rbe, rbo, rce, rco)
    rlo, rle = swap_odd(lo, "lane"), swap_even(le, "lane")
    rmbo, rmbe = swap_odd(mbo, "band"), swap_even(mbe, "band")

    lext, lbe, lbo = call(
        coarse_bands, [coarse, band_coarse, band_coarse], [VM] * 3, name="coarse_bands"
    )(cl, rle, rlo)
    rlbo, rlbe = swap_odd(lbo, "band"), swap_even(lbe, "band")
    v3, wext = call(
        between,
        [fine, coarse],
        [VM] * 6,
        [coarse_buf],
        aliases={0: 0},
        flops=10**7,
        name="between",
    )(v3, mext, rmbe, rmbo, rle, rlo)

    (out,) = call(
        after,
        [own],
        [VM] * 7,
        [coarse_buf] * 3 + [pltpu.VMEM((N + 8, L), f32), fine_buf, fine_buf],
        flops=10**8,
        name="after",
        inner=False,
    )(v3, f, w, wext, lext, rlbe, rlbo)
    return out


def solution(mesh):
    spec = P("band", "lane", None)
    return jax.shard_map(
        shards, mesh=mesh, in_specs=(spec, spec, spec), out_specs=spec, check_vma=False
    )
```

```python
import functools

import jax
import jax.numpy as jnp
from jax import lax
from jax.experimental import pallas as pl
from jax.experimental.pallas import tpu as pltpu
from jax.sharding import PartitionSpec as P


RATIO = 4
BEFORE = 3
AFTER = 2
INNER = 13

N = 64
C = N // RATIO
L = 128
DS = BEFORE + 1
DF = DS - 1
DEPTH = DS + 2 * DF
AT_LOAD, AT_MASS = N * DS, N * (DS + DF)
FINE = N * DEPTH
R0, C0 = DS, 12
R1, C1 = R0 + N, C0 + N
ROWS, COLS = R1 + DS, C1 + 12
FULL = ((C0 - 4, C0 + 20), (C0 + 20, C0 + 44), (C0 + 44, C0 + 68))
EDGES = ((C0 - 4, C0 + 4), (C1 - 4, C1 + 4))
H = INNER
CR0, CC0 = H, 20
CR, CCOLS = C + 2 * H, 56
WIDTHS = [C + 2 * (H + 1 - j) for j in range(1, H + 1)]
STARTS = [sum(WIDTHS[:k]) for k in range(H)]
BAND_COARSE = -(-sum(WIDTHS) // 8) * 8
BAND_RIM = N + 8
LANE_COARSE = C * H
PIECES = 4
FIT = 16 * 2**20

f32 = jnp.float32


def parity(axis):
    return lax.rem(lax.axis_index(axis), 2) == 0


def either(test, one, other):
    @pl.when(test)
    def _():
        one()

    @pl.when(jnp.logical_not(test))
    def _():
        other()


def sds(*shape):
    return jax.ShapeDtypeStruct(shape, f32)


VM = pl.BlockSpec(memory_space=pltpu.VMEM)
HBM = pl.BlockSpec(memory_space=pltpu.HBM)


def call(body, outs, ins, scratch=(), aliases=None, flops=10**6, result=False):
    return pl.pallas_call(
        body,
        out_shape=outs[:result] + [pltpu.VMEM(o.shape, o.dtype) for o in outs[result:]],
        in_specs=ins,
        out_specs=[HBM] * result + [VM] * (len(outs) - result),
        scratch_shapes=list(scratch),
        input_output_aliases=aliases or {},
        compiler_params=pltpu.CompilerParams(vmem_limit_bytes=FIT),
        cost_estimate=pl.CostEstimate(flops=flops, bytes_accessed=8 * 10**6, transcendentals=0),
    )


def loop(count, per, body):
    def turn(g, carry):
        for k in range(per):
            body(g * per + k)
        return carry

    lax.fori_loop(0, count // per, turn, 0)


def gather_columns(line, row):
    line[...] = row
    total = line[pl.ds(0, C, stride=RATIO), :]
    for k in range(1, RATIO):
        total = total + line[pl.ds(k, C, stride=RATIO), :]
    return total * (1.0 / RATIO)


def pack_fine(load, start, mass_hbm, m_even, m_odd, b_even, b_odd, mass, cm, edges, c_odd, side, line, sem_side, sem_mass, sem_band):
    whole = pltpu.make_async_copy(mass_hbm, mass, sem_mass.at[0])
    copies = []
    for k, src in enumerate((start, load)):
        for s, at in enumerate((0, N - 8)):
            copies.append(
                pltpu.make_async_copy(src.at[:, pl.ds(at, 8)], side.at[k, s], sem_side.at[k, s])
            )
    even = parity("band")
    bands = []
    for which, (dst, bottom) in enumerate(((b_even, even), (b_odd, jnp.logical_not(even)))):
        at = 0
        for k, (src, depth) in enumerate(((start, DS), (load, DF), (mass_hbm, DF))):
            first = jnp.where(bottom, N - depth, 0)
            bands.append(
                pltpu.make_async_copy(
                    src.at[pl.ds(first, depth)], dst.at[pl.ds(at, depth)], sem_band.at[which, k]
                )
            )
            at += depth
    for c in copies:
        c.start()
    whole.start()
    for c in bands:
        c.start()
    for c in copies:
        c.wait()

    def pack(right, left):
        def group(g, carry):
            for k, (depth, field) in enumerate(((DS, 0), (DF, AT_LOAD))):
                base = pl.multiple_of(g * (8 * depth), 8)
                for r in range(8):
                    at = field + base + r * depth
                    right[pl.ds(at, depth), :] = side[k, 1, g * 8 + r, 8 - depth :, :]
                    left[pl.ds(at, depth), :] = side[k, 0, g * 8 + r, :depth, :]
            return carry

        lax.fori_loop(0, N // 8, group, 0)

    lane_even = parity("lane")
    either(lane_even, lambda: pack(m_even, m_odd), lambda: pack(m_odd, m_even))
    whole.wait()

    def pack_mass(right, left):
        def group(g, carry):
            base = pl.multiple_of(g * (8 * DF), 8)
            for half in range(2):
                total = None
                for k in range(RATIO):
                    r = half * RATIO + k
                    at = AT_MASS + base + r * DF
                    row = mass[g * 8 + r]
                    total = row if total is None else total + row
                    right[pl.ds(at, DF), :] = row[N - DF :, :]
                    left[pl.ds(at, DF), :] = row[:DF, :]
                cm[2 * g + half] = gather_columns(line.at[half], total)
            return carry

        lax.fori_loop(0, N // 8, group, 0)

    either(
        lane_even,
        lambda: pack_mass(m_even, m_odd),
        lambda: pack_mass(m_odd, m_even),
    )
    for i in range(C):
        row = cm[i]
        edges[i * H : (i + 1) * H, :] = row[:H, :]
        edges[LANE_COARSE + i * H : LANE_COARSE + (i + 1) * H, :] = row[C - H :, :]

    def odd_side(first):
        c_odd[...] = edges[first : first + LANE_COARSE, :]

    either(lane_even, lambda: odd_side(0), lambda: odd_side(LANE_COARSE))
    for c in bands:
        c.wait()


def pack_corners(m_even, m_odd, token, c_even, c_odd):
    del token

    def fill(left, right):
        def put(dst, bottom):
            at = 0
            for src in (left, right):
                for field, depth in ((0, DS), (AT_LOAD, DF), (AT_MASS, DF)):
                    lo, size = field + (N - DF) * depth * bottom, DF * depth
                    dst[at : at + size, :] = src[lo : lo + size, :]
                    at += size

        either(
            parity("band"),
            lambda: (put(c_even, 1), put(c_odd, 0)),
            lambda: (put(c_even, 0), put(c_odd, 1)),
        )

    either(parity("lane"), lambda: fill(m_odd, m_even), lambda: fill(m_even, m_odd))


def pack_coarse_lanes(own, right, left, at):
    for i in range(C):
        lo = at + i * H
        row = own[i]
        right[lo : lo + H, :] = row[C - H :, :]
        left[lo : lo + H, :] = row[:H, :]


def place_coarse_lanes(ext, left, right, at_left=0, at_right=0):
    for i in range(C):
        ext[CR0 + i, CC0 - H : CC0, :] = left[at_left + i * H : at_left + (i + 1) * H, :]
        ext[CR0 + i, CC0 + C : CC0 + C + H, :] = right[at_right + i * H : at_right + (i + 1) * H, :]


def pack_coarse_bands(ext, down, up):
    for j in range(1, H + 1):
        reach, at, wide = H + 1 - j, STARTS[j - 1], WIDTHS[j - 1]
        cols = slice(CC0 - reach, CC0 + C + reach)
        down[at : at + wide, :] = ext[CR0 + C - j, cols, :]
        up[at : at + wide, :] = ext[CR0 + j - 1, cols, :]
    for dst in (down, up):
        dst[sum(WIDTHS) : BAND_COARSE, :] = jnp.zeros((BAND_COARSE - sum(WIDTHS), L), f32)


def place_coarse_bands(ext, above, below):
    for j in range(1, H + 1):
        reach, at, wide = H + 1 - j, STARTS[j - 1], WIDTHS[j - 1]
        cols = slice(CC0 - reach, CC0 + C + reach)
        ext[CR0 - j, cols, :] = above[at : at + wide, :]
        ext[CR0 + C + j - 1, cols, :] = below[at : at + wide, :]


def weight(mass):
    return 0.8 / (4.0 + mass)


def sweep_rows(src, dst, w, f, first, last, segments, per=4):
    def some(r, count):
        for lo, hi in segments:
            line = [src[r - 1 + k, lo:hi, :] for k in range(count + 2)]
            for k in range(count):
                q = r + k
                around = (line[k] + line[k + 2]) + (
                    src[q, lo - 1 : hi - 1, :] + src[q, lo + 1 : hi + 1, :]
                )
                dst[q, lo:hi, :] = 0.2 * line[k + 1] + w[q, lo:hi, :] * (f[q, lo:hi, :] + around)

    whole = (last - first) // per
    if whole > 1:

        def group(g, carry):
            some(first + g * per, per)
            return carry

        lax.fori_loop(0, whole, group, 0)
        first = first + whole * per
    for r in range(first, last, per):
        some(r, min(per, last - r))


def defect_sum(v, f, a4, first, lo, hi):
    total = None
    line = [v[first - 1 + k, lo:hi, :] for k in range(RATIO + 2)]
    for k in range(RATIO):
        q = first + k
        around = (line[k] + line[k + 2]) + (v[q, lo - 1 : hi - 1, :] + v[q, lo + 1 : hi + 1, :])
        one = (f[q, lo:hi, :] + around) - a4[q, lo:hi, :] * line[k + 1]
        total = one if total is None else total + one
    return total


def prepare(load, start, mass, u, f, w, a4, v1, v2, v3, cl, token, load_in, start_in, line, sems):
    copies = [
        pltpu.make_async_copy(load, load_in, sems.at[0]),
        pltpu.make_async_copy(start, start_in, sems.at[1]),
    ]
    for c in copies:
        c.start()

    def weights(r):
        a = 4.0 + mass[r]
        a4[R0 + r, C0:C1, :] = a
        w[R0 + r, C0:C1, :] = 0.8 / a

    loop(N, 2, weights)
    for c in copies:
        c.wait()

    def place(r):
        f[R0 + r, C0:C1, :] = load_in[r]
        u[R0 + r, C0:C1, :] = start_in[r]

    loop(N, 2, place)
    sweep_rows(u, v1, w, f, R0 + 1, R1 - 1, FULL)
    sweep_rows(v1, v2, w, f, R0 + 2, R1 - 2, FULL)
    sweep_rows(v2, v3, w, f, R0 + 3, R1 - 3, FULL)

    def block(i, carry):
        cl[i] = gather_columns(line, defect_sum(v3, f, a4, R0 + RATIO * i, C0, C1))
        return carry

    lax.fori_loop(1, C - 1, block, 0)
    token[...] = jnp.zeros((8, L), f32)


def before(u_in, f_in, w_in, v1_in, v2_in, v3_in, cl_in, a4, re, ro, be, bo, ce, co, u, f, w, v1, v2, v3, cl, l_even, l_odd, rim_even, rim_odd, wl, wr, wc, line):
    del u_in, f_in, w_in, v1_in, v2_in, v3_in, cl_in

    def lanes(left, right):
        for msg, out in ((left, wl), (right, wr)):
            out[...] = weight(msg[AT_MASS:FINE, :])
        for msg, out, cs, cf in ((left, wl, C0 - DS, C0 - DF), (right, wr, C1, C1)):

            def group(g, carry):
                s0, f0 = pl.multiple_of(g * (8 * DS), 8), pl.multiple_of(g * (8 * DF), 8)
                for r in range(8):
                    row = R0 + g * 8 + r
                    u[row, cs : cs + DS, :] = msg[pl.ds(s0 + r * DS, DS), :]
                    f[row, cf : cf + DF, :] = msg[pl.ds(AT_LOAD + f0 + r * DF, DF), :]
                    w[row, cf : cf + DF, :] = out[pl.ds(f0 + r * DF, DF), :]
                return carry

            lax.fori_loop(0, N // 8, group, 0)

    lane_even, band_even = parity("lane"), parity("band")
    either(lane_even, lambda: lanes(ro, re), lambda: lanes(re, ro))

    def bands(above, below, above_c, below_c):
        own = slice(C0, C1)
        for msg, row in ((above, R0), (below, R1)):
            first = row - DS if row == R0 else row
            for k in range(DS):
                u[first + k, own, :] = msg[k]
            first = row - DF if row == R0 else row
            for k in range(DF):
                f[first + k, own, :] = msg[DS + k]
                w[first + k, own, :] = weight(msg[DS + DF + k])
        for msg, first in ((above_c, R0 - DF), (below_c, R1)):
            half = DF * DEPTH
            wc[...] = weight(msg[...])
            for at, cs, cf in ((0, C0 - DS, C0 - DF), (half, C1, C1)):
                for k in range(DF):
                    row = first + k
                    s0, l0, m0 = at + k * DS, at + DF * DS + k * DF, at + DF * (DS + DF) + k * DF
                    u[row, cs : cs + DS, :] = msg[s0 : s0 + DS, :]
                    f[row, cf : cf + DF, :] = msg[l0 : l0 + DF, :]
                    w[row, cf : cf + DF, :] = wc[m0 : m0 + DF, :]

    either(band_even, lambda: bands(bo, be, co, ce), lambda: bands(be, bo, ce, co))

    for src, dst, k in ((u, v1, 1), (v1, v2, 2), (v2, v3, 3)):
        reach = BEFORE + 1 - k
        sweep_rows(src, dst, w, f, R0 - reach, R0 + k, FULL)
        sweep_rows(src, dst, w, f, R1 - k, R1 + reach, FULL)
        sweep_rows(src, dst, w, f, R0 + k, R1 - k, EDGES)

    for i in (0, C - 1):
        cl[i] = gather_columns(line, defect_sum(v3, f, a4, R0 + RATIO * i, C0, C1))

    def rims(i, carry):
        row = R0 + RATIO * i
        left = defect_sum(v3, f, a4, row, C0 - 4, C0 + 4)
        right = defect_sum(v3, f, a4, row, C1 - 4, C1 + 4)
        cl[i, 0:1, :] = jnp.sum(left[4:8, :], axis=0, keepdims=True) * (1.0 / RATIO)
        cl[i, C - 1 : C, :] = jnp.sum(right[0:4, :], axis=0, keepdims=True) * (1.0 / RATIO)
        return carry

    lax.fori_loop(1, C - 1, rims, 0)

    def out_lanes(right, left):
        pack_coarse_lanes(cl, right, left, 0)

        def group(g, carry):
            base = pl.multiple_of(g * 8, 8)
            for r in range(8):
                row = R0 + g * 8 + r
                right[pl.ds(LANE_COARSE + base + r, 1), :] = v3[row, C1 - 2 : C1 - 1, :]
                left[pl.ds(LANE_COARSE + base + r, 1), :] = v3[row, C0 + 1 : C0 + 2, :]
            return carry

        lax.fori_loop(0, N // 8, group, 0)

    either(lane_even, lambda: out_lanes(l_even, l_odd), lambda: out_lanes(l_odd, l_even))

    def out_bands(down, up):
        for dst, rim, edge in ((down, R1 - 2, R1 - 1), (up, R0 + 1, R0)):
            at = 0
            dst[at : at + N, :] = v3[rim, C0:C1, :]
            dst[at + N : at + N + 8, :] = jnp.zeros((8, L), f32)
            dst[at + N : at + N + 1, :] = v3[edge, C0 - 1 : C0, :]
            dst[at + N + 1 : at + N + 2, :] = v3[edge, C1 : C1 + 1, :]

    either(band_even, lambda: out_bands(rim_even, rim_odd), lambda: out_bands(rim_odd, rim_even))


def relay(edges, out):
    def put(first):
        out[...] = edges[first : first + LANE_COARSE, :]

    either(parity("lane"), lambda: put(LANE_COARSE), lambda: put(0))


def far(lane, lanes):
    at = lax.rem(lane, lanes // 2)
    return (at == 0) | (at == lanes // 2 - 1)


def mass_bands(lanes, cm, edges, near, across, mext, b_even, b_odd):
    for i in range(C):
        mext[CR0 + i, CC0 : CC0 + C, :] = cm[i]

    def place(odd):
        either(
            parity("lane"),
            lambda: place_coarse_lanes(mext, odd, edges),
            lambda: place_coarse_lanes(mext, edges, odd, LANE_COARSE),
        )

    either(far(lax.axis_index("lane"), lanes), lambda: place(across), lambda: place(near))
    either(
        parity("band"),
        lambda: pack_coarse_bands(mext, b_even, b_odd),
        lambda: pack_coarse_bands(mext, b_odd, b_even),
    )


def coarse_bands(cl, re, ro, rim_even, rim_odd, lext, b_even, b_odd):
    for i in range(C):
        lext[CR0 + i, CC0 : CC0 + C, :] = cl[i]
    either(
        parity("lane"),
        lambda: place_coarse_lanes(lext, ro, re),
        lambda: place_coarse_lanes(lext, re, ro),
    )
    either(
        parity("band"),
        lambda: pack_coarse_bands(lext, b_even, b_odd),
        lambda: pack_coarse_bands(lext, b_odd, b_even),
    )
    b_even[BAND_COARSE:, :] = rim_even[...]
    b_odd[BAND_COARSE:, :] = rim_odd[...]


def between(v_in, mext, mbe, mbo, le, lo, v, wext, ext):
    del v_in

    def lanes(left, right):
        def group(g, carry):
            base = pl.multiple_of(g * 8, 8)
            for r in range(8):
                row = R0 + g * 8 + r
                v[row, C0 - 2 : C0 - 1, :] = left[pl.ds(LANE_COARSE + base + r, 1), :]
                v[row, C1 + 1 : C1 + 2, :] = right[pl.ds(LANE_COARSE + base + r, 1), :]
            return carry

        lax.fori_loop(0, N // 8, group, 0)

    either(parity("lane"), lambda: lanes(lo, le), lambda: lanes(le, lo))
    span = slice(CC0 - H, CC0 + C + H)
    for i in range(C):
        ext[CR0 + i, span, :] = mext[CR0 + i, span, :]

    def bands(above, below):
        place_coarse_bands(ext, above, below)

    either(parity("band"), lambda: bands(mbo, mbe), lambda: bands(mbe, mbo))

    def weights(r):
        wext[r] = weight(ext[r])

    loop(CR, 2, weights)


def after(v_in, f, w, wext, lext_in, lbe, lbo, result, v, lext, a, b, wide, t, s, out, sems):
    span = slice(CC0 - H, CC0 + C + H)
    for i in range(C):
        lext[CR0 + i, span, :] = lext_in[CR0 + i, span, :]
    del v_in

    def bands(above, below):
        place_coarse_bands(lext, above, below)
        for msg, rim, edge in ((above, R0 - 2, R0 - 1), (below, R1 + 1, R1)):
            at = BAND_COARSE
            v[rim, C0:C1, :] = msg[at : at + N, :]
            v[edge, C0 - 1 : C0, :] = msg[at + N : at + N + 1, :]
            v[edge, C1 : C1 + 1, :] = msg[at + N + 1 : at + N + 2, :]

    either(parity("band"), lambda: bands(lbo, lbe), lambda: bands(lbe, lbo))

    def first(r):
        a[r] = wext[r] * lext[r]

    loop(CR, 2, first)
    src, dst = a, b
    for k in range(1, INNER):
        segments = ((8, 24), (24, 48)) if k <= 8 else ((16, 40),)
        sweep_rows(src, dst, wext, lext, k, CR - k, segments)
        src, dst = dst, src
    for i in range(-1, C + 1):
        row = src[CR0 + i, CC0 - 1 : CC0 + C + 1, :]
        for k in range(RATIO):
            wide[pl.ds(k, C + 2, stride=RATIO), :] = row
        for k in range(RATIO):
            q = i * RATIO + k
            if -AFTER <= q < N + AFTER:
                t[R0 + q, C0 - 4 : C1 + 4, :] = v[R0 + q, C0 - 4 : C1 + 4, :] + wide[...]
    sweep_rows(t, s, w, f, R0 - 1, R1 + 1, FULL, per=2)

    def last(r, carry):
        for lo, hi in ((0, 32), (32, 64)):
            line = [s[R0 + 4 * r - 1 + k, C0 + lo : C0 + hi, :] for k in range(6)]
            for k in range(4):
                q = R0 + 4 * r + k
                around = (line[k] + line[k + 2]) + (
                    s[q, C0 + lo - 1 : C0 + hi - 1, :] + s[q, C0 + lo + 1 : C0 + hi + 1, :]
                )
                out[4 * r + k, lo:hi, :] = 0.2 * line[k + 1] + w[q, C0 + lo : C0 + hi, :] * (
                    f[q, C0 + lo : C0 + hi, :] + around
                )
        return carry

    copies = []
    for piece in range(PIECES):
        rows = N // PIECES
        lax.fori_loop(piece * rows // 4, (piece + 1) * rows // 4, last, 0)
        span = pl.ds(piece * rows, rows)
        copies.append(pltpu.make_async_copy(out.at[span], result.at[span], sems.at[piece]))
        copies[-1].start()
    for c in copies:
        c.wait()


def swap_even(x, axis):
    n = lax.axis_size(axis)
    return lax.ppermute(x, axis, [(i, i ^ 1) for i in range(n)])


def swap_odd(x, axis):
    n = lax.axis_size(axis)
    return lax.ppermute(x, axis, [(i, (i + 1) % n if i % 2 else (i - 1) % n) for i in range(n)])


def shards(load, start, mass):
    load, start, mass = (pltpu.with_memory_space_constraint(x, pltpu.HBM) for x in (load, start, mass))
    dma = pltpu.SemaphoreType.DMA
    own, fine = sds(N, N, L), sds(ROWS, COLS, L)
    corner = sds(2 * DF * DEPTH, L)
    lane_msg, band_msg = sds(FINE, L), sds(DEPTH, N, L)
    rim, lane_mass = sds(BAND_RIM, L), sds(LANE_COARSE, L)
    lane_coarse, band_coarse = sds(LANE_COARSE + N, L), sds(BAND_COARSE, L)
    band_both = sds(BAND_COARSE + BAND_RIM, L)
    coarse, own_coarse = sds(CR, CCOLS, L), sds(C, C, L)
    coarse_buf, fine_buf = pltpu.VMEM((CR, CCOLS, L), f32), pltpu.VMEM((ROWS, COLS, L), f32)
    own_buf, line = pltpu.VMEM((N, N, L), f32), pltpu.VMEM((N, L), f32)

    me, mo, be, bo, mass_in, cm, edges, cmo = call(
        pack_fine,
        [lane_msg, lane_msg, band_msg, band_msg, own, own_coarse, sds(2 * LANE_COARSE, L), lane_mass],
        [HBM] * 3,
        [pltpu.VMEM((2, 2, N, 8, L), f32), pltpu.VMEM((2, N, L), f32), dma((2, 2)), dma((1,)), dma((2, 3))],
    )(load, start, mass)
    rbo, rbe = swap_odd(bo, "band"), swap_even(be, "band")
    ro, re = swap_odd(mo, "lane"), swap_even(me, "lane")

    n = lax.axis_size("lane")
    half = n // 2
    redges = swap_even(edges, "lane")
    pairs = [(i, i + 1) for i in range(1, n - 1, 2) if i != half - 1]
    rnear = lax.ppermute(cmo, "lane", pairs + [(j, i) for i, j in pairs])
    (hand,) = call(relay, [lane_mass], [VM])(redges)
    pairs = [(half - 2, half + 1), (n - 2, 1)]
    rhand = lax.ppermute(hand, "lane", pairs + [(j, i) for i, j in pairs])
    racross = swap_even(rhand, "lane")

    u, f, w, a4, v1, v2, v3, cl, token = call(
        prepare,
        [fine] * 7 + [own_coarse, sds(8, L)],
        [HBM, HBM, VM],
        [own_buf, own_buf, line, dma((2,))],
        flops=10**8,
    )(load, start, mass_in)

    ce, co = call(pack_corners, [corner, corner], [VM] * 3)(re, ro, token)
    rco, rce = swap_odd(co, "band"), swap_even(ce, "band")

    mext, mbe, mbo = call(
        functools.partial(mass_bands, n), [coarse, band_coarse, band_coarse], [VM] * 4
    )(cm, redges, rnear, racross)
    rmbo, rmbe = swap_odd(mbo, "band"), swap_even(mbe, "band")

    u, f, w, v1, v2, v3, cl, le, lo, rime, rimo = call(
        before,
        [fine] * 6 + [own_coarse, lane_coarse, lane_coarse, rim, rim],
        [VM] * 14,
        [pltpu.VMEM((N * DF, L), f32), pltpu.VMEM((N * DF, L), f32), pltpu.VMEM(corner.shape, f32), line],
        aliases={k: k for k in range(7)},
        flops=10**8,
    )(u, f, w, v1, v2, v3, cl, a4, re, ro, rbe, rbo, rce, rco)
    rlo, rle = swap_odd(lo, "lane"), swap_even(le, "lane")
    lext, lbe, lbo = call(
        coarse_bands, [coarse, band_both, band_both], [VM] * 5
    )(cl, rle, rlo, rime, rimo)
    rlbo, rlbe = swap_odd(lbo, "band"), swap_even(lbe, "band")
    v3, wext = call(
        between, [fine, coarse], [VM] * 6, [coarse_buf], aliases={0: 0}, flops=10**7
    )(v3, mext, rmbe, rmbo, rle, rlo)

    out, _ = call(
        after,
        [own, fine],
        [VM] * 7,
        [coarse_buf] * 3 + [pltpu.VMEM((N + 8, L), f32), fine_buf, fine_buf, own_buf, dma((PIECES,))],
        flops=10**8,
        aliases={0: 1},
        result=True,
    )(v3, f, w, wext, lext, rlbe, rlbo)
    return out


def solution(mesh):
    spec = P("band", "lane", None)

    return jax.shard_map(
        shards, mesh=mesh, in_specs=(spec, spec, spec), out_specs=spec, check_vma=False
    )
```

```python
import functools

import jax
import jax.numpy as jnp
from jax import lax
from jax.experimental import pallas as pl
from jax.experimental.pallas import tpu as pltpu
from jax.sharding import PartitionSpec as P


RATIO = 4
BEFORE = 3
AFTER = 2
INNER = 13

N = 64
C = N // RATIO
L = 128
DS = BEFORE + 1
DF = DS - 1
DEPTH = DS + 2 * DF
AT_LOAD, AT_MASS = N * DS, N * (DS + DF)
FINE = N * DEPTH
R0, C0 = DS, 12
R1, C1 = R0 + N, C0 + N
ROWS, COLS = R1 + DS, C1 + 12
FULL = ((C0 - 4, C0 + 20), (C0 + 20, C0 + 44), (C0 + 44, C0 + 68))
EDGES = ((C0 - 4, C0 + 4), (C1 - 4, C1 + 4))
H = INNER
CR0, CC0 = H, 20
CR, CCOLS = C + 2 * H, 56
WIDTHS = [C + 2 * (H + 1 - j) for j in range(1, H + 1)]
STARTS = [sum(WIDTHS[:k]) for k in range(H)]
BAND_COARSE = -(-sum(WIDTHS) // 8) * 8
BAND_OWN = C * H
BAND_RIM = N + 8
BAND_LATE = -(-H * (H + 1) // 8) * 8
REACHES = [(j, H + 1 - j, (j - 1) * (2 * H + 2) - (j - 1) * j) for j in range(1, H + 1)]
LANE_COARSE = C * H
PIECES = 4
FIT = 16 * 2**20

f32 = jnp.float32


def parity(axis):
    return lax.rem(lax.axis_index(axis), 2) == 0


def either(test, one, other):
    @pl.when(test)
    def _():
        one()

    @pl.when(jnp.logical_not(test))
    def _():
        other()


def sds(*shape):
    return jax.ShapeDtypeStruct(shape, f32)


VM = pl.BlockSpec(memory_space=pltpu.VMEM)
HBM = pl.BlockSpec(memory_space=pltpu.HBM)


def call(body, outs, ins, scratch=(), aliases=None, flops=10**6, result=False):
    return pl.pallas_call(
        body,
        out_shape=outs[:result] + [pltpu.VMEM(o.shape, o.dtype) for o in outs[result:]],
        in_specs=ins,
        out_specs=[HBM] * result + [VM] * (len(outs) - result),
        scratch_shapes=list(scratch),
        input_output_aliases=aliases or {},
        compiler_params=pltpu.CompilerParams(vmem_limit_bytes=FIT),
        cost_estimate=pl.CostEstimate(flops=flops, bytes_accessed=8 * 10**6, transcendentals=0),
    )


def loop(count, per, body):
    def turn(g, carry):
        for k in range(per):
            body(g * per + k)
        return carry

    lax.fori_loop(0, count // per, turn, 0)


def gather_columns(line, row):
    line[...] = row
    total = line[pl.ds(0, C, stride=RATIO), :]
    for k in range(1, RATIO):
        total = total + line[pl.ds(k, C, stride=RATIO), :]
    return total * (1.0 / RATIO)


def pack_fine(load, start, mass_hbm, m_even, m_odd, b_even, b_odd, mass, cm, edges, c_odd, side, line, sem_side, sem_mass, sem_band):
    whole = pltpu.make_async_copy(mass_hbm, mass, sem_mass.at[0])
    copies = []
    for k, src in enumerate((start, load)):
        for s, at in enumerate((0, N - 8)):
            copies.append(
                pltpu.make_async_copy(src.at[:, pl.ds(at, 8)], side.at[k, s], sem_side.at[k, s])
            )
    even = parity("band")
    bands = []
    for which, (dst, bottom) in enumerate(((b_even, even), (b_odd, jnp.logical_not(even)))):
        at = 0
        for k, (src, depth) in enumerate(((start, DS), (load, DF), (mass_hbm, DF))):
            first = jnp.where(bottom, N - depth, 0)
            bands.append(
                pltpu.make_async_copy(
                    src.at[pl.ds(first, depth)], dst.at[pl.ds(at, depth)], sem_band.at[which, k]
                )
            )
            at += depth
    for c in copies:
        c.start()
    whole.start()
    for c in bands:
        c.start()
    for c in copies:
        c.wait()

    def pack(right, left):
        def group(g, carry):
            for k, (depth, field) in enumerate(((DS, 0), (DF, AT_LOAD))):
                base = pl.multiple_of(g * (8 * depth), 8)
                for r in range(8):
                    at = field + base + r * depth
                    right[pl.ds(at, depth), :] = side[k, 1, g * 8 + r, 8 - depth :, :]
                    left[pl.ds(at, depth), :] = side[k, 0, g * 8 + r, :depth, :]
            return carry

        lax.fori_loop(0, N // 8, group, 0)

    lane_even = parity("lane")
    either(lane_even, lambda: pack(m_even, m_odd), lambda: pack(m_odd, m_even))
    whole.wait()

    def pack_mass(right, left):
        def group(g, carry):
            base = pl.multiple_of(g * (8 * DF), 8)
            for half in range(2):
                total = None
                for k in range(RATIO):
                    r = half * RATIO + k
                    at = AT_MASS + base + r * DF
                    row = mass[g * 8 + r]
                    total = row if total is None else total + row
                    right[pl.ds(at, DF), :] = row[N - DF :, :]
                    left[pl.ds(at, DF), :] = row[:DF, :]
                cm[2 * g + half] = gather_columns(line.at[half], total)
            return carry

        lax.fori_loop(0, N // 8, group, 0)

    either(
        lane_even,
        lambda: pack_mass(m_even, m_odd),
        lambda: pack_mass(m_odd, m_even),
    )
    for i in range(C):
        row = cm[i]
        edges[i * H : (i + 1) * H, :] = row[:H, :]
        edges[LANE_COARSE + i * H : LANE_COARSE + (i + 1) * H, :] = row[C - H :, :]

    def odd_side(first):
        c_odd[...] = edges[first : first + LANE_COARSE, :]

    either(lane_even, lambda: odd_side(0), lambda: odd_side(LANE_COARSE))
    for c in bands:
        c.wait()


def pack_corners(m_even, m_odd, token, c_even, c_odd):
    del token

    def fill(left, right):
        def put(dst, bottom):
            at = 0
            for src in (left, right):
                for field, depth in ((0, DS), (AT_LOAD, DF), (AT_MASS, DF)):
                    lo, size = field + (N - DF) * depth * bottom, DF * depth
                    dst[at : at + size, :] = src[lo : lo + size, :]
                    at += size

        either(
            parity("band"),
            lambda: (put(c_even, 1), put(c_odd, 0)),
            lambda: (put(c_even, 0), put(c_odd, 1)),
        )

    either(parity("lane"), lambda: fill(m_odd, m_even), lambda: fill(m_even, m_odd))


def pack_coarse_lanes(own, right, left, at):
    for i in range(C):
        lo = at + i * H
        row = own[i]
        right[lo : lo + H, :] = row[C - H :, :]
        left[lo : lo + H, :] = row[:H, :]


def place_coarse_lanes(ext, left, right, at_left=0, at_right=0):
    for i in range(C):
        ext[CR0 + i, CC0 - H : CC0, :] = left[at_left + i * H : at_left + (i + 1) * H, :]
        ext[CR0 + i, CC0 + C : CC0 + C + H, :] = right[at_right + i * H : at_right + (i + 1) * H, :]


def pack_coarse_bands(ext, down, up):
    for j in range(1, H + 1):
        reach, at, wide = H + 1 - j, STARTS[j - 1], WIDTHS[j - 1]
        cols = slice(CC0 - reach, CC0 + C + reach)
        down[at : at + wide, :] = ext[CR0 + C - j, cols, :]
        up[at : at + wide, :] = ext[CR0 + j - 1, cols, :]
    for dst in (down, up):
        dst[sum(WIDTHS) : BAND_COARSE, :] = jnp.zeros((BAND_COARSE - sum(WIDTHS), L), f32)


def place_coarse_bands(ext, above, below):
    for j in range(1, H + 1):
        reach, at, wide = H + 1 - j, STARTS[j - 1], WIDTHS[j - 1]
        cols = slice(CC0 - reach, CC0 + C + reach)
        ext[CR0 - j, cols, :] = above[at : at + wide, :]
        ext[CR0 + C + j - 1, cols, :] = below[at : at + wide, :]


def pack_late(ext, down, up):
    for j, reach, at in REACHES:
        for dst, row in ((down, CR0 + C - j), (up, CR0 + j - 1)):
            dst[at : at + reach, :] = ext[row, CC0 - reach : CC0, :]
            dst[at + reach : at + 2 * reach, :] = ext[row, CC0 + C : CC0 + C + reach, :]
    for dst in (down, up):
        dst[H * (H + 1) :, :] = jnp.zeros((BAND_LATE - H * (H + 1), L), f32)


def place_late(ext, above, below):
    for j, reach, at in REACHES:
        for msg, row in ((above, CR0 - j), (below, CR0 + C + j - 1)):
            ext[row, CC0 - reach : CC0, :] = msg[at : at + reach, :]
            ext[row, CC0 + C : CC0 + C + reach, :] = msg[at + reach : at + 2 * reach, :]


def weight(mass):
    return 0.8 / (4.0 + mass)


def sweep_rows(src, dst, w, f, first, last, segments, per=4):
    def some(r, count):
        for lo, hi in segments:
            line = [src[r - 1 + k, lo:hi, :] for k in range(count + 2)]
            for k in range(count):
                q = r + k
                around = (line[k] + line[k + 2]) + (
                    src[q, lo - 1 : hi - 1, :] + src[q, lo + 1 : hi + 1, :]
                )
                dst[q, lo:hi, :] = 0.2 * line[k + 1] + w[q, lo:hi, :] * (f[q, lo:hi, :] + around)

    whole = (last - first) // per
    if whole > 1:

        def group(g, carry):
            some(first + g * per, per)
            return carry

        lax.fori_loop(0, whole, group, 0)
        first = first + whole * per
    for r in range(first, last, per):
        some(r, min(per, last - r))


def defect_sum(v, f, a4, first, lo, hi):
    total = None
    line = [v[first - 1 + k, lo:hi, :] for k in range(RATIO + 2)]
    for k in range(RATIO):
        q = first + k
        around = (line[k] + line[k + 2]) + (v[q, lo - 1 : hi - 1, :] + v[q, lo + 1 : hi + 1, :])
        one = (f[q, lo:hi, :] + around) - a4[q, lo:hi, :] * line[k + 1]
        total = one if total is None else total + one
    return total


def prepare(load, start, mass, u, f, w, a4, v1, v2, v3, cl, token, load_in, start_in, line, sems):
    copies = [
        pltpu.make_async_copy(load, load_in, sems.at[0]),
        pltpu.make_async_copy(start, start_in, sems.at[1]),
    ]
    for c in copies:
        c.start()

    def weights(r):
        a = 4.0 + mass[r]
        a4[R0 + r, C0:C1, :] = a
        w[R0 + r, C0:C1, :] = 0.8 / a

    loop(N, 2, weights)
    for c in copies:
        c.wait()

    def place(r):
        f[R0 + r, C0:C1, :] = load_in[r]
        u[R0 + r, C0:C1, :] = start_in[r]

    loop(N, 2, place)
    sweep_rows(u, v1, w, f, R0 + 1, R1 - 1, FULL)
    sweep_rows(v1, v2, w, f, R0 + 2, R1 - 2, FULL)
    sweep_rows(v2, v3, w, f, R0 + 3, R1 - 3, FULL)

    def block(i, carry):
        cl[i] = gather_columns(line, defect_sum(v3, f, a4, R0 + RATIO * i, C0, C1))
        return carry

    lax.fori_loop(1, C - 1, block, 0)
    token[...] = jnp.zeros((8, L), f32)


def before(u_in, f_in, w_in, v1_in, v2_in, v3_in, cl_in, a4, re, ro, be, bo, ce, co, u, f, w, v1, v2, v3, cl, l_even, l_odd, rim_even, rim_odd, wl, wr, wc, line):
    del u_in, f_in, w_in, v1_in, v2_in, v3_in, cl_in

    def lanes(left, right):
        for msg, out in ((left, wl), (right, wr)):
            out[...] = weight(msg[AT_MASS:FINE, :])
        for msg, out, cs, cf in ((left, wl, C0 - DS, C0 - DF), (right, wr, C1, C1)):

            def group(g, carry):
                s0, f0 = pl.multiple_of(g * (8 * DS), 8), pl.multiple_of(g * (8 * DF), 8)
                for r in range(8):
                    row = R0 + g * 8 + r
                    u[row, cs : cs + DS, :] = msg[pl.ds(s0 + r * DS, DS), :]
                    f[row, cf : cf + DF, :] = msg[pl.ds(AT_LOAD + f0 + r * DF, DF), :]
                    w[row, cf : cf + DF, :] = out[pl.ds(f0 + r * DF, DF), :]
                return carry

            lax.fori_loop(0, N // 8, group, 0)

    lane_even, band_even = parity("lane"), parity("band")
    either(lane_even, lambda: lanes(ro, re), lambda: lanes(re, ro))

    def bands(above, below, above_c, below_c):
        own = slice(C0, C1)
        for msg, row in ((above, R0), (below, R1)):
            first = row - DS if row == R0 else row
            for k in range(DS):
                u[first + k, own, :] = msg[k]
            first = row - DF if row == R0 else row
            for k in range(DF):
                f[first + k, own, :] = msg[DS + k]
                w[first + k, own, :] = weight(msg[DS + DF + k])
        for msg, first in ((above_c, R0 - DF), (below_c, R1)):
            half = DF * DEPTH
            wc[...] = weight(msg[...])
            for at, cs, cf in ((0, C0 - DS, C0 - DF), (half, C1, C1)):
                for k in range(DF):
                    row = first + k
                    s0, l0, m0 = at + k * DS, at + DF * DS + k * DF, at + DF * (DS + DF) + k * DF
                    u[row, cs : cs + DS, :] = msg[s0 : s0 + DS, :]
                    f[row, cf : cf + DF, :] = msg[l0 : l0 + DF, :]
                    w[row, cf : cf + DF, :] = wc[m0 : m0 + DF, :]

    either(band_even, lambda: bands(bo, be, co, ce), lambda: bands(be, bo, ce, co))

    for src, dst, k in ((u, v1, 1), (v1, v2, 2), (v2, v3, 3)):
        reach = BEFORE + 1 - k
        sweep_rows(src, dst, w, f, R0 - reach, R0 + k, FULL)
        sweep_rows(src, dst, w, f, R1 - k, R1 + reach, FULL)
        sweep_rows(src, dst, w, f, R0 + k, R1 - k, EDGES)

    for i in (0, C - 1):
        cl[i] = gather_columns(line, defect_sum(v3, f, a4, R0 + RATIO * i, C0, C1))

    def rims(i, carry):
        row = R0 + RATIO * i
        left = defect_sum(v3, f, a4, row, C0 - 4, C0 + 4)
        right = defect_sum(v3, f, a4, row, C1 - 4, C1 + 4)
        cl[i, 0:1, :] = jnp.sum(left[4:8, :], axis=0, keepdims=True) * (1.0 / RATIO)
        cl[i, C - 1 : C, :] = jnp.sum(right[0:4, :], axis=0, keepdims=True) * (1.0 / RATIO)
        return carry

    lax.fori_loop(1, C - 1, rims, 0)

    def out_lanes(right, left):
        pack_coarse_lanes(cl, right, left, 0)

        def group(g, carry):
            base = pl.multiple_of(g * 8, 8)
            for r in range(8):
                row = R0 + g * 8 + r
                right[pl.ds(LANE_COARSE + base + r, 1), :] = v3[row, C1 - 2 : C1 - 1, :]
                left[pl.ds(LANE_COARSE + base + r, 1), :] = v3[row, C0 + 1 : C0 + 2, :]
            return carry

        lax.fori_loop(0, N // 8, group, 0)

    either(lane_even, lambda: out_lanes(l_even, l_odd), lambda: out_lanes(l_odd, l_even))

    def out_bands(down, up):
        for j in range(1, H + 1):
            down[(j - 1) * C : j * C, :] = cl[C - j]
            up[(j - 1) * C : j * C, :] = cl[j - 1]
        for dst, rim, edge in ((down, R1 - 2, R1 - 1), (up, R0 + 1, R0)):
            at = BAND_OWN
            dst[at : at + N, :] = v3[rim, C0:C1, :]
            dst[at + N : at + N + 8, :] = jnp.zeros((8, L), f32)
            dst[at + N : at + N + 1, :] = v3[edge, C0 - 1 : C0, :]
            dst[at + N + 1 : at + N + 2, :] = v3[edge, C1 : C1 + 1, :]

    either(band_even, lambda: out_bands(rim_even, rim_odd), lambda: out_bands(rim_odd, rim_even))


def relay(edges, out):
    def put(first):
        out[...] = edges[first : first + LANE_COARSE, :]

    either(parity("lane"), lambda: put(LANE_COARSE), lambda: put(0))


def far(lane, lanes):
    at = lax.rem(lane, lanes // 2)
    return (at == 0) | (at == lanes // 2 - 1)


def mass_bands(lanes, cm, edges, near, across, mext, b_even, b_odd):
    for i in range(C):
        mext[CR0 + i, CC0 : CC0 + C, :] = cm[i]

    def place(odd):
        either(
            parity("lane"),
            lambda: place_coarse_lanes(mext, odd, edges),
            lambda: place_coarse_lanes(mext, edges, odd, LANE_COARSE),
        )

    either(far(lax.axis_index("lane"), lanes), lambda: place(across), lambda: place(near))
    either(
        parity("band"),
        lambda: pack_coarse_bands(mext, b_even, b_odd),
        lambda: pack_coarse_bands(mext, b_odd, b_even),
    )


def coarse_bands(cl, re, ro, lext, b_even, b_odd):
    for i in range(C):
        lext[CR0 + i, CC0 : CC0 + C, :] = cl[i]
    either(
        parity("lane"),
        lambda: place_coarse_lanes(lext, ro, re),
        lambda: place_coarse_lanes(lext, re, ro),
    )
    either(
        parity("band"),
        lambda: pack_late(lext, b_even, b_odd),
        lambda: pack_late(lext, b_odd, b_even),
    )


def between(v_in, lext_in, mext, mbe, mbo, le, lo, rbe, rbo, v, lext, wext, ext):
    del v_in, lext_in

    def lanes(left, right):
        def group(g, carry):
            base = pl.multiple_of(g * 8, 8)
            for r in range(8):
                row = R0 + g * 8 + r
                v[row, C0 - 2 : C0 - 1, :] = left[pl.ds(LANE_COARSE + base + r, 1), :]
                v[row, C1 + 1 : C1 + 2, :] = right[pl.ds(LANE_COARSE + base + r, 1), :]
            return carry

        lax.fori_loop(0, N // 8, group, 0)

    either(parity("lane"), lambda: lanes(lo, le), lambda: lanes(le, lo))
    span = slice(CC0 - H, CC0 + C + H)
    for i in range(C):
        ext[CR0 + i, span, :] = mext[CR0 + i, span, :]

    def own(above, below):
        for j in range(1, H + 1):
            lext[CR0 - j, CC0 : CC0 + C, :] = above[(j - 1) * C : j * C, :]
            lext[CR0 + C + j - 1, CC0 : CC0 + C, :] = below[(j - 1) * C : j * C, :]
        for msg, rim, edge in ((above, R0 - 2, R0 - 1), (below, R1 + 1, R1)):
            at = BAND_OWN
            v[rim, C0:C1, :] = msg[at : at + N, :]
            v[edge, C0 - 1 : C0, :] = msg[at + N : at + N + 1, :]
            v[edge, C1 : C1 + 1, :] = msg[at + N + 1 : at + N + 2, :]

    either(parity("band"), lambda: own(rbo, rbe), lambda: own(rbe, rbo))

    def bands(above, below):
        place_coarse_bands(ext, above, below)

    either(parity("band"), lambda: bands(mbo, mbe), lambda: bands(mbe, mbo))

    def weights(r):
        wext[r] = weight(ext[r])

    loop(CR, 2, weights)


def after(v, f, w, wext, lext_in, lbe, lbo, result, lext, a, b, wide, t, s, out, sems):
    del lext_in
    either(
        parity("band"),
        lambda: place_late(lext, lbo, lbe),
        lambda: place_late(lext, lbe, lbo),
    )

    def first(r):
        a[r] = wext[r] * lext[r]

    loop(CR, 2, first)
    src, dst = a, b
    for k in range(1, INNER):
        segments = ((8, 24), (24, 48)) if k <= 8 else ((16, 40),)
        sweep_rows(src, dst, wext, lext, k, CR - k, segments)
        src, dst = dst, src
    for i in range(-1, C + 1):
        row = src[CR0 + i, CC0 - 1 : CC0 + C + 1, :]
        for k in range(RATIO):
            wide[pl.ds(k, C + 2, stride=RATIO), :] = row
        for k in range(RATIO):
            q = i * RATIO + k
            if -AFTER <= q < N + AFTER:
                t[R0 + q, C0 - 4 : C1 + 4, :] = v[R0 + q, C0 - 4 : C1 + 4, :] + wide[...]
    sweep_rows(t, s, w, f, R0 - 1, R1 + 1, FULL, per=2)

    def last(r, carry):
        for lo, hi in ((0, 32), (32, 64)):
            line = [s[R0 + 4 * r - 1 + k, C0 + lo : C0 + hi, :] for k in range(6)]
            for k in range(4):
                q = R0 + 4 * r + k
                around = (line[k] + line[k + 2]) + (
                    s[q, C0 + lo - 1 : C0 + hi - 1, :] + s[q, C0 + lo + 1 : C0 + hi + 1, :]
                )
                out[4 * r + k, lo:hi, :] = 0.2 * line[k + 1] + w[q, C0 + lo : C0 + hi, :] * (
                    f[q, C0 + lo : C0 + hi, :] + around
                )
        return carry

    copies = []
    for piece in range(PIECES):
        rows = N // PIECES
        lax.fori_loop(piece * rows // 4, (piece + 1) * rows // 4, last, 0)
        span = pl.ds(piece * rows, rows)
        copies.append(pltpu.make_async_copy(out.at[span], result.at[span], sems.at[piece]))
        copies[-1].start()
    for c in copies:
        c.wait()


def swap_even(x, axis):
    n = lax.axis_size(axis)
    return lax.ppermute(x, axis, [(i, i ^ 1) for i in range(n)])


def swap_odd(x, axis):
    n = lax.axis_size(axis)
    return lax.ppermute(x, axis, [(i, (i + 1) % n if i % 2 else (i - 1) % n) for i in range(n)])


def shards(load, start, mass):
    load, start, mass = (pltpu.with_memory_space_constraint(x, pltpu.HBM) for x in (load, start, mass))
    dma = pltpu.SemaphoreType.DMA
    own, fine = sds(N, N, L), sds(ROWS, COLS, L)
    corner = sds(2 * DF * DEPTH, L)
    lane_msg, band_msg = sds(FINE, L), sds(DEPTH, N, L)
    early, lane_mass = sds(BAND_OWN + BAND_RIM, L), sds(LANE_COARSE, L)
    lane_coarse, band_coarse = sds(LANE_COARSE + N, L), sds(BAND_COARSE, L)
    band_late = sds(BAND_LATE, L)
    coarse, own_coarse = sds(CR, CCOLS, L), sds(C, C, L)
    coarse_buf, fine_buf = pltpu.VMEM((CR, CCOLS, L), f32), pltpu.VMEM((ROWS, COLS, L), f32)
    own_buf, line = pltpu.VMEM((N, N, L), f32), pltpu.VMEM((N, L), f32)

    me, mo, be, bo, mass_in, cm, edges, cmo = call(
        pack_fine,
        [lane_msg, lane_msg, band_msg, band_msg, own, own_coarse, sds(2 * LANE_COARSE, L), lane_mass],
        [HBM] * 3,
        [pltpu.VMEM((2, 2, N, 8, L), f32), pltpu.VMEM((2, N, L), f32), dma((2, 2)), dma((1,)), dma((2, 3))],
    )(load, start, mass)
    rbo, rbe = swap_odd(bo, "band"), swap_even(be, "band")
    ro, re = swap_odd(mo, "lane"), swap_even(me, "lane")

    n = lax.axis_size("lane")
    half = n // 2
    redges = swap_even(edges, "lane")
    pairs = [(i, i + 1) for i in range(1, n - 1, 2) if i != half - 1]
    rnear = lax.ppermute(cmo, "lane", pairs + [(j, i) for i, j in pairs])
    (hand,) = call(relay, [lane_mass], [VM])(redges)
    pairs = [(half - 2, half + 1), (n - 2, 1)]
    rhand = lax.ppermute(hand, "lane", pairs + [(j, i) for i, j in pairs])
    racross = swap_even(rhand, "lane")

    u, f, w, a4, v1, v2, v3, cl, token = call(
        prepare,
        [fine] * 7 + [own_coarse, sds(8, L)],
        [HBM, HBM, VM],
        [own_buf, own_buf, line, dma((2,))],
        flops=10**8,
    )(load, start, mass_in)

    ce, co = call(pack_corners, [corner, corner], [VM] * 3)(re, ro, token)
    rco, rce = swap_odd(co, "band"), swap_even(ce, "band")

    mext, mbe, mbo = call(
        functools.partial(mass_bands, n), [coarse, band_coarse, band_coarse], [VM] * 4
    )(cm, redges, rnear, racross)
    rmbo, rmbe = swap_odd(mbo, "band"), swap_even(mbe, "band")

    u, f, w, v1, v2, v3, cl, le, lo, rime, rimo = call(
        before,
        [fine] * 6 + [own_coarse, lane_coarse, lane_coarse, early, early],
        [VM] * 14,
        [pltpu.VMEM((N * DF, L), f32), pltpu.VMEM((N * DF, L), f32), pltpu.VMEM(corner.shape, f32), line],
        aliases={k: k for k in range(7)},
        flops=10**8,
    )(u, f, w, v1, v2, v3, cl, a4, re, ro, rbe, rbo, rce, rco)
    rlo, rle = swap_odd(lo, "lane"), swap_even(le, "lane")
    rrimo, rrime = swap_odd(rimo, "band"), swap_even(rime, "band")
    lext, lbe, lbo = call(coarse_bands, [coarse, band_late, band_late], [VM] * 3)(cl, rle, rlo)
    rlbo, rlbe = swap_odd(lbo, "band"), swap_even(lbe, "band")
    v3, lext, wext = call(
        between, [fine, coarse, coarse], [VM] * 9, [coarse_buf], aliases={0: 0, 1: 1}, flops=10**7
    )(v3, lext, mext, rmbe, rmbo, rle, rlo, rrime, rrimo)

    out, _ = call(
        after,
        [own, coarse],
        [VM] * 7,
        [coarse_buf] * 2 + [pltpu.VMEM((N + 8, L), f32), fine_buf, fine_buf, own_buf, dma((PIECES,))],
        flops=10**8,
        aliases={4: 1},
        result=True,
    )(v3, f, w, wext, lext, rlbe, rlbo)
    return out


def solution(mesh):
    spec = P("band", "lane", None)

    return jax.shard_map(
        shards, mesh=mesh, in_specs=(spec, spec, spec), out_specs=spec, check_vma=False
    )
```

```python
import functools

import jax
import jax.numpy as jnp
from jax import lax
from jax.experimental import pallas as pl
from jax.experimental.pallas import tpu as pltpu
from jax.sharding import PartitionSpec as P


RATIO = 4
BEFORE = 3
AFTER = 2
INNER = 13

N = 64
C = N // RATIO
L = 128
DS = BEFORE + 1
DF = DS - 1
DEPTH = DS + 2 * DF
AT_LOAD, AT_MASS = N * DS, N * (DS + DF)
FINE = N * DEPTH
R0, C0 = DS, 12
R1, C1 = R0 + N, C0 + N
ROWS, COLS = R1 + DS, C1 + 12
FULL = ((C0 - 4, C0 + 20), (C0 + 20, C0 + 44), (C0 + 44, C0 + 68))
EDGES = ((C0 - 4, C0 + 4), (C1 - 4, C1 + 4))
H = INNER
CR0, CC0 = H, 20
CR, CCOLS = C + 2 * H, 56
WIDTHS = [C + 2 * (H + 1 - j) for j in range(1, H + 1)]
STARTS = [sum(WIDTHS[:k]) for k in range(H)]
BAND_COARSE = -(-sum(WIDTHS) // 8) * 8
BAND_OWN = C * H
BAND_RIM = N + 8
BAND_LATE = -(-H * (H + 1) // 8) * 8
REACHES = [(j, H + 1 - j, (j - 1) * (2 * H + 2) - (j - 1) * j) for j in range(1, H + 1)]
LANE_COARSE = C * H
PIECES = 16
FIT = 16 * 2**20

f32 = jnp.float32


def parity(axis):
    return lax.rem(lax.axis_index(axis), 2) == 0


def either(test, one, other):
    @pl.when(test)
    def _():
        one()

    @pl.when(jnp.logical_not(test))
    def _():
        other()


def sds(*shape):
    return jax.ShapeDtypeStruct(shape, f32)


VM = pl.BlockSpec(memory_space=pltpu.VMEM)
HBM = pl.BlockSpec(memory_space=pltpu.HBM)


def call(body, outs, ins, scratch=(), aliases=None, flops=10**6, result=False):
    return pl.pallas_call(
        body,
        out_shape=outs[:result] + [pltpu.VMEM(o.shape, o.dtype) for o in outs[result:]],
        in_specs=ins,
        out_specs=[HBM] * result + [VM] * (len(outs) - result),
        scratch_shapes=list(scratch),
        input_output_aliases=aliases or {},
        compiler_params=pltpu.CompilerParams(vmem_limit_bytes=FIT),
        cost_estimate=pl.CostEstimate(flops=flops, bytes_accessed=8 * 10**6, transcendentals=0),
    )


def loop(count, per, body):
    def turn(g, carry):
        for k in range(per):
            body(g * per + k)
        return carry

    lax.fori_loop(0, count // per, turn, 0)


def gather_columns(line, row):
    line[...] = row
    total = line[pl.ds(0, C, stride=RATIO), :]
    for k in range(1, RATIO):
        total = total + line[pl.ds(k, C, stride=RATIO), :]
    return total * (1.0 / RATIO)


def pack_fine(load, start, mass_hbm, m_even, m_odd, b_even, b_odd, mass, cm, edges, c_odd, side, line, sem_side, sem_mass, sem_band):
    whole = pltpu.make_async_copy(mass_hbm, mass, sem_mass.at[0])
    copies = []
    for k, src in enumerate((start, load)):
        for s, at in enumerate((0, N - 8)):
            copies.append(
                pltpu.make_async_copy(src.at[:, pl.ds(at, 8)], side.at[k, s], sem_side.at[k, s])
            )
    even = parity("band")
    bands = []
    for which, (dst, bottom) in enumerate(((b_even, even), (b_odd, jnp.logical_not(even)))):
        at = 0
        for k, (src, depth) in enumerate(((start, DS), (load, DF), (mass_hbm, DF))):
            first = jnp.where(bottom, N - depth, 0)
            bands.append(
                pltpu.make_async_copy(
                    src.at[pl.ds(first, depth)], dst.at[pl.ds(at, depth)], sem_band.at[which, k]
                )
            )
            at += depth
    for c in copies:
        c.start()
    whole.start()
    for c in bands:
        c.start()
    for c in copies:
        c.wait()

    def pack(right, left):
        def group(g, carry):
            for k, (depth, field) in enumerate(((DS, 0), (DF, AT_LOAD))):
                base = pl.multiple_of(g * (8 * depth), 8)
                for r in range(8):
                    at = field + base + r * depth
                    right[pl.ds(at, depth), :] = side[k, 1, g * 8 + r, 8 - depth :, :]
                    left[pl.ds(at, depth), :] = side[k, 0, g * 8 + r, :depth, :]
            return carry

        lax.fori_loop(0, N // 8, group, 0)

    lane_even = parity("lane")
    either(lane_even, lambda: pack(m_even, m_odd), lambda: pack(m_odd, m_even))
    whole.wait()

    def pack_mass(right, left):
        def group(g, carry):
            base = pl.multiple_of(g * (8 * DF), 8)
            for half in range(2):
                total = None
                for k in range(RATIO):
                    r = half * RATIO + k
                    at = AT_MASS + base + r * DF
                    row = mass[g * 8 + r]
                    total = row if total is None else total + row
                    right[pl.ds(at, DF), :] = row[N - DF :, :]
                    left[pl.ds(at, DF), :] = row[:DF, :]
                cm[2 * g + half] = gather_columns(line.at[half], total)
            return carry

        lax.fori_loop(0, N // 8, group, 0)

    either(
        lane_even,
        lambda: pack_mass(m_even, m_odd),
        lambda: pack_mass(m_odd, m_even),
    )
    for i in range(C):
        row = cm[i]
        edges[i * H : (i + 1) * H, :] = row[:H, :]
        edges[LANE_COARSE + i * H : LANE_COARSE + (i + 1) * H, :] = row[C - H :, :]

    def odd_side(first):
        c_odd[...] = edges[first : first + LANE_COARSE, :]

    either(lane_even, lambda: odd_side(0), lambda: odd_side(LANE_COARSE))
    for c in bands:
        c.wait()


def pack_corners(m_even, m_odd, token, c_even, c_odd):
    del token

    def fill(left, right):
        def put(dst, bottom):
            at = 0
            for src in (left, right):
                for field, depth in ((0, DS), (AT_LOAD, DF), (AT_MASS, DF)):
                    lo, size = field + (N - DF) * depth * bottom, DF * depth
                    dst[at : at + size, :] = src[lo : lo + size, :]
                    at += size

        either(
            parity("band"),
            lambda: (put(c_even, 1), put(c_odd, 0)),
            lambda: (put(c_even, 0), put(c_odd, 1)),
        )

    either(parity("lane"), lambda: fill(m_odd, m_even), lambda: fill(m_even, m_odd))


def pack_coarse_lanes(own, right, left, at):
    for i in range(C):
        lo = at + i * H
        row = own[i]
        right[lo : lo + H, :] = row[C - H :, :]
        left[lo : lo + H, :] = row[:H, :]


def place_coarse_lanes(ext, left, right, at_left=0, at_right=0):
    for i in range(C):
        ext[CR0 + i, CC0 - H : CC0, :] = left[at_left + i * H : at_left + (i + 1) * H, :]
        ext[CR0 + i, CC0 + C : CC0 + C + H, :] = right[at_right + i * H : at_right + (i + 1) * H, :]


def pack_coarse_bands(ext, down, up):
    for j in range(1, H + 1):
        reach, at, wide = H + 1 - j, STARTS[j - 1], WIDTHS[j - 1]
        cols = slice(CC0 - reach, CC0 + C + reach)
        down[at : at + wide, :] = ext[CR0 + C - j, cols, :]
        up[at : at + wide, :] = ext[CR0 + j - 1, cols, :]
    for dst in (down, up):
        dst[sum(WIDTHS) : BAND_COARSE, :] = jnp.zeros((BAND_COARSE - sum(WIDTHS), L), f32)


def place_coarse_bands(ext, above, below):
    for j in range(1, H + 1):
        reach, at, wide = H + 1 - j, STARTS[j - 1], WIDTHS[j - 1]
        cols = slice(CC0 - reach, CC0 + C + reach)
        ext[CR0 - j, cols, :] = above[at : at + wide, :]
        ext[CR0 + C + j - 1, cols, :] = below[at : at + wide, :]


def pack_late(ext, down, up):
    for j, reach, at in REACHES:
        for dst, row in ((down, CR0 + C - j), (up, CR0 + j - 1)):
            dst[at : at + reach, :] = ext[row, CC0 - reach : CC0, :]
            dst[at + reach : at + 2 * reach, :] = ext[row, CC0 + C : CC0 + C + reach, :]
    for dst in (down, up):
        dst[H * (H + 1) :, :] = jnp.zeros((BAND_LATE - H * (H + 1), L), f32)


def place_late(ext, a, wext, above, below):
    for j, reach, at in REACHES:
        for msg, row in ((above, CR0 - j), (below, CR0 + C + j - 1)):
            for lo, first in ((at, CC0 - reach), (at + reach, CC0 + C)):
                cols = slice(first, first + reach)
                values = msg[lo : lo + reach, :]
                ext[row, cols, :] = values
                a[row, cols, :] = wext[row, cols, :] * values


def weight(mass):
    return 0.8 / (4.0 + mass)


def sweep_rows(src, dst, w, f, first, last, segments, per=4):
    def some(r, count):
        for lo, hi in segments:
            line = [src[r - 1 + k, lo:hi, :] for k in range(count + 2)]
            for k in range(count):
                q = r + k
                around = (line[k] + line[k + 2]) + (
                    src[q, lo - 1 : hi - 1, :] + src[q, lo + 1 : hi + 1, :]
                )
                dst[q, lo:hi, :] = 0.2 * line[k + 1] + w[q, lo:hi, :] * (f[q, lo:hi, :] + around)

    whole = (last - first) // per
    if whole > 1:

        def group(g, carry):
            some(first + g * per, per)
            return carry

        lax.fori_loop(0, whole, group, 0)
        first = first + whole * per
    for r in range(first, last, per):
        some(r, min(per, last - r))


def defect_sum(v, f, a4, first, lo, hi):
    total = None
    line = [v[first - 1 + k, lo:hi, :] for k in range(RATIO + 2)]
    for k in range(RATIO):
        q = first + k
        around = (line[k] + line[k + 2]) + (v[q, lo - 1 : hi - 1, :] + v[q, lo + 1 : hi + 1, :])
        one = (f[q, lo:hi, :] + around) - a4[q, lo:hi, :] * line[k + 1]
        total = one if total is None else total + one
    return total


def prepare(load, start, mass, u, f, w, a4, v1, v2, v3, cl, token, load_in, start_in, line, sems):
    copies = [
        pltpu.make_async_copy(load, load_in, sems.at[0]),
        pltpu.make_async_copy(start, start_in, sems.at[1]),
    ]
    for c in copies:
        c.start()

    def weights(r):
        a = 4.0 + mass[r]
        a4[R0 + r, C0:C1, :] = a
        w[R0 + r, C0:C1, :] = 0.8 / a

    loop(N, 2, weights)
    for c in copies:
        c.wait()

    def place(r):
        f[R0 + r, C0:C1, :] = load_in[r]
        u[R0 + r, C0:C1, :] = start_in[r]

    loop(N, 2, place)
    sweep_rows(u, v1, w, f, R0 + 1, R1 - 1, FULL)
    sweep_rows(v1, v2, w, f, R0 + 2, R1 - 2, FULL)
    sweep_rows(v2, v3, w, f, R0 + 3, R1 - 3, FULL)

    def block(i, carry):
        cl[i] = gather_columns(line, defect_sum(v3, f, a4, R0 + RATIO * i, C0, C1))
        return carry

    lax.fori_loop(1, C - 1, block, 0)
    token[...] = jnp.zeros((8, L), f32)


def from_lanes(u_in, f_in, w_in, v1_in, v2_in, v3_in, cl_in, a4, re, ro, u, f, w, v1, v2, v3, cl, wl, wr):
    del u_in, f_in, w_in, v1_in, v2_in, v3_in, cl_in

    def lanes(left, right):
        for msg, out in ((left, wl), (right, wr)):
            out[...] = weight(msg[AT_MASS:FINE, :])
        for msg, out, cs, cf in ((left, wl, C0 - DS, C0 - DF), (right, wr, C1, C1)):

            def group(g, carry):
                s0, f0 = pl.multiple_of(g * (8 * DS), 8), pl.multiple_of(g * (8 * DF), 8)
                for r in range(8):
                    row = R0 + g * 8 + r
                    u[row, cs : cs + DS, :] = msg[pl.ds(s0 + r * DS, DS), :]
                    f[row, cf : cf + DF, :] = msg[pl.ds(AT_LOAD + f0 + r * DF, DF), :]
                    w[row, cf : cf + DF, :] = out[pl.ds(f0 + r * DF, DF), :]
                return carry

            lax.fori_loop(0, N // 8, group, 0)

    either(parity("lane"), lambda: lanes(ro, re), lambda: lanes(re, ro))
    for src, dst, k in ((u, v1, 1), (v1, v2, 2), (v2, v3, 3)):
        sweep_rows(src, dst, w, f, R0 + k, R1 - k, EDGES)

    def rims(i, carry):
        row = R0 + RATIO * i
        left = defect_sum(v3, f, a4, row, C0 - 4, C0 + 4)
        right = defect_sum(v3, f, a4, row, C1 - 4, C1 + 4)
        cl[i, 0:1, :] = jnp.sum(left[4:8, :], axis=0, keepdims=True) * (1.0 / RATIO)
        cl[i, C - 1 : C, :] = jnp.sum(right[0:4, :], axis=0, keepdims=True) * (1.0 / RATIO)
        return carry

    lax.fori_loop(1, C - 1, rims, 0)


def before(u_in, f_in, w_in, v1_in, v2_in, v3_in, cl_in, a4, be, bo, ce, co, u, f, w, v1, v2, v3, cl, l_even, l_odd, rim_even, rim_odd, wc, line):
    del u_in, f_in, w_in, v1_in, v2_in, v3_in, cl_in

    lane_even, band_even = parity("lane"), parity("band")

    def bands(above, below, above_c, below_c):
        own = slice(C0, C1)
        for msg, row in ((above, R0), (below, R1)):
            first = row - DS if row == R0 else row
            for k in range(DS):
                u[first + k, own, :] = msg[k]
            first = row - DF if row == R0 else row
            for k in range(DF):
                f[first + k, own, :] = msg[DS + k]
                w[first + k, own, :] = weight(msg[DS + DF + k])
        for msg, first in ((above_c, R0 - DF), (below_c, R1)):
            half = DF * DEPTH
            wc[...] = weight(msg[...])
            for at, cs, cf in ((0, C0 - DS, C0 - DF), (half, C1, C1)):
                for k in range(DF):
                    row = first + k
                    s0, l0, m0 = at + k * DS, at + DF * DS + k * DF, at + DF * (DS + DF) + k * DF
                    u[row, cs : cs + DS, :] = msg[s0 : s0 + DS, :]
                    f[row, cf : cf + DF, :] = msg[l0 : l0 + DF, :]
                    w[row, cf : cf + DF, :] = wc[m0 : m0 + DF, :]

    either(band_even, lambda: bands(bo, be, co, ce), lambda: bands(be, bo, ce, co))

    for src, dst, k in ((u, v1, 1), (v1, v2, 2), (v2, v3, 3)):
        reach = BEFORE + 1 - k
        sweep_rows(src, dst, w, f, R0 - reach, R0 + k, FULL)
        sweep_rows(src, dst, w, f, R1 - k, R1 + reach, FULL)

    for i in (0, C - 1):
        cl[i] = gather_columns(line, defect_sum(v3, f, a4, R0 + RATIO * i, C0, C1))

    def out_lanes(right, left):
        pack_coarse_lanes(cl, right, left, 0)

        def group(g, carry):
            base = pl.multiple_of(g * 8, 8)
            for r in range(8):
                row = R0 + g * 8 + r
                right[pl.ds(LANE_COARSE + base + r, 1), :] = v3[row, C1 - 2 : C1 - 1, :]
                left[pl.ds(LANE_COARSE + base + r, 1), :] = v3[row, C0 + 1 : C0 + 2, :]
            return carry

        lax.fori_loop(0, N // 8, group, 0)

    either(lane_even, lambda: out_lanes(l_even, l_odd), lambda: out_lanes(l_odd, l_even))

    def out_bands(down, up):
        for j in range(1, H + 1):
            down[(j - 1) * C : j * C, :] = cl[C - j]
            up[(j - 1) * C : j * C, :] = cl[j - 1]
        for dst, rim, edge in ((down, R1 - 2, R1 - 1), (up, R0 + 1, R0)):
            at = BAND_OWN
            dst[at : at + N, :] = v3[rim, C0:C1, :]
            dst[at + N : at + N + 8, :] = jnp.zeros((8, L), f32)
            dst[at + N : at + N + 1, :] = v3[edge, C0 - 1 : C0, :]
            dst[at + N + 1 : at + N + 2, :] = v3[edge, C1 : C1 + 1, :]

    either(band_even, lambda: out_bands(rim_even, rim_odd), lambda: out_bands(rim_odd, rim_even))


def relay(edges, out):
    def put(first):
        out[...] = edges[first : first + LANE_COARSE, :]

    either(parity("lane"), lambda: put(LANE_COARSE), lambda: put(0))


def far(lane, lanes):
    at = lax.rem(lane, lanes // 2)
    return (at == 0) | (at == lanes // 2 - 1)


def mass_bands(lanes, cm, edges, near, across, mext, b_even, b_odd):
    for i in range(C):
        mext[CR0 + i, CC0 : CC0 + C, :] = cm[i]

    def place(odd):
        either(
            parity("lane"),
            lambda: place_coarse_lanes(mext, odd, edges),
            lambda: place_coarse_lanes(mext, edges, odd, LANE_COARSE),
        )

    either(far(lax.axis_index("lane"), lanes), lambda: place(across), lambda: place(near))
    either(
        parity("band"),
        lambda: pack_coarse_bands(mext, b_even, b_odd),
        lambda: pack_coarse_bands(mext, b_odd, b_even),
    )


def coarse_bands(cl, re, ro, lext, b_even, b_odd):
    for i in range(C):
        lext[CR0 + i, CC0 : CC0 + C, :] = cl[i]
    either(
        parity("lane"),
        lambda: place_coarse_lanes(lext, ro, re),
        lambda: place_coarse_lanes(lext, re, ro),
    )
    either(
        parity("band"),
        lambda: pack_late(lext, b_even, b_odd),
        lambda: pack_late(lext, b_odd, b_even),
    )


def between(v_in, lext_in, mext, mbe, mbo, le, lo, rbe, rbo, v, lext, wext, a, ext):
    del v_in, lext_in

    def lanes(left, right):
        def group(g, carry):
            base = pl.multiple_of(g * 8, 8)
            for r in range(8):
                row = R0 + g * 8 + r
                v[row, C0 - 2 : C0 - 1, :] = left[pl.ds(LANE_COARSE + base + r, 1), :]
                v[row, C1 + 1 : C1 + 2, :] = right[pl.ds(LANE_COARSE + base + r, 1), :]
            return carry

        lax.fori_loop(0, N // 8, group, 0)

    either(parity("lane"), lambda: lanes(lo, le), lambda: lanes(le, lo))
    span = slice(CC0 - H, CC0 + C + H)
    for i in range(C):
        ext[CR0 + i, span, :] = mext[CR0 + i, span, :]

    def own(above, below):
        for j in range(1, H + 1):
            lext[CR0 - j, CC0 : CC0 + C, :] = above[(j - 1) * C : j * C, :]
            lext[CR0 + C + j - 1, CC0 : CC0 + C, :] = below[(j - 1) * C : j * C, :]
        for msg, rim, edge in ((above, R0 - 2, R0 - 1), (below, R1 + 1, R1)):
            at = BAND_OWN
            v[rim, C0:C1, :] = msg[at : at + N, :]
            v[edge, C0 - 1 : C0, :] = msg[at + N : at + N + 1, :]
            v[edge, C1 : C1 + 1, :] = msg[at + N + 1 : at + N + 2, :]

    either(parity("band"), lambda: own(rbo, rbe), lambda: own(rbe, rbo))

    def bands(above, below):
        place_coarse_bands(ext, above, below)

    either(parity("band"), lambda: bands(mbo, mbe), lambda: bands(mbe, mbo))

    def weights(r):
        wc = weight(ext[r])
        wext[r] = wc
        a[r] = wc * lext[r]

    loop(CR, 2, weights)


def after(v, f, w, wext, lext_in, a_in, lbe, lbo, result, lext, a, b, wide, t, s, out, sems):
    del lext_in, a_in
    either(
        parity("band"),
        lambda: place_late(lext, a, wext, lbo, lbe),
        lambda: place_late(lext, a, wext, lbe, lbo),
    )

    src, dst = a, b
    for k in range(1, INNER):
        first = CC0 - H + k
        wide_by = -(-(CR - 2 * k) // 8) * 8
        segments = ((first, first + 16), (first + 16, first + wide_by)) if wide_by > 24 else ((first, first + 24),)
        sweep_rows(src, dst, wext, lext, k, CR - k, segments)
        src, dst = dst, src

    def correct(i):
        row = src[CR0 + i, CC0 - 1 : CC0 + C + 1, :]
        for k in range(RATIO):
            wide[pl.ds(k, C + 2, stride=RATIO), :] = row
        for k in range(RATIO):
            q = i * RATIO + k
            if -AFTER <= q < N + AFTER:
                t[R0 + q, C0 - 4 : C1 + 4, :] = v[R0 + q, C0 - 4 : C1 + 4, :] + wide[...]

    def last(r, carry):
        for lo, hi in ((0, 32), (32, 64)):
            line = [s[R0 + 4 * r - 1 + k, C0 + lo : C0 + hi, :] for k in range(6)]
            for k in range(4):
                q = R0 + 4 * r + k
                around = (line[k] + line[k + 2]) + (
                    s[q, C0 + lo - 1 : C0 + hi - 1, :] + s[q, C0 + lo + 1 : C0 + hi + 1, :]
                )
                out[4 * r + k, lo:hi, :] = 0.2 * line[k + 1] + w[q, C0 + lo : C0 + hi, :] * (
                    f[q, C0 + lo : C0 + hi, :] + around
                )
        return carry

    copies = []
    rows = N // PIECES
    corrected, swept = -1, R0 - 1
    for piece in range(PIECES):
        end = (piece + 1) * rows
        upto = min(C, (end + 1) // RATIO)
        for i in range(corrected, upto + 1):
            correct(i)
        corrected = upto + 1
        sweep_rows(t, s, w, f, swept, R0 + end + 1, FULL)
        swept = R0 + end + 1
        lax.fori_loop(piece * rows // 4, end // 4, last, 0)
        span = pl.ds(piece * rows, rows)
        copies.append(pltpu.make_async_copy(out.at[span], result.at[span], sems.at[piece]))
        copies[-1].start()
    for c in copies:
        c.wait()


def swap_even(x, axis):
    n = lax.axis_size(axis)
    return lax.ppermute(x, axis, [(i, i ^ 1) for i in range(n)])


def swap_odd(x, axis):
    n = lax.axis_size(axis)
    return lax.ppermute(x, axis, [(i, (i + 1) % n if i % 2 else (i - 1) % n) for i in range(n)])


def shards(load, start, mass):
    load, start, mass = (pltpu.with_memory_space_constraint(x, pltpu.HBM) for x in (load, start, mass))
    dma = pltpu.SemaphoreType.DMA
    own, fine = sds(N, N, L), sds(ROWS, COLS, L)
    corner = sds(2 * DF * DEPTH, L)
    lane_msg, band_msg = sds(FINE, L), sds(DEPTH, N, L)
    early, lane_mass = sds(BAND_OWN + BAND_RIM, L), sds(LANE_COARSE, L)
    lane_coarse, band_coarse = sds(LANE_COARSE + N, L), sds(BAND_COARSE, L)
    band_late = sds(BAND_LATE, L)
    coarse, own_coarse = sds(CR, CCOLS, L), sds(C, C, L)
    coarse_buf, fine_buf = pltpu.VMEM((CR, CCOLS, L), f32), pltpu.VMEM((ROWS, COLS, L), f32)
    own_buf, line = pltpu.VMEM((N, N, L), f32), pltpu.VMEM((N, L), f32)

    me, mo, be, bo, mass_in, cm, edges, cmo = call(
        pack_fine,
        [lane_msg, lane_msg, band_msg, band_msg, own, own_coarse, sds(2 * LANE_COARSE, L), lane_mass],
        [HBM] * 3,
        [pltpu.VMEM((2, 2, N, 8, L), f32), pltpu.VMEM((2, N, L), f32), dma((2, 2)), dma((1,)), dma((2, 3))],
    )(load, start, mass)
    rbo, rbe = swap_odd(bo, "band"), swap_even(be, "band")
    ro, re = swap_odd(mo, "lane"), swap_even(me, "lane")

    n = lax.axis_size("lane")
    half = n // 2
    redges = swap_even(edges, "lane")
    pairs = [(i, i + 1) for i in range(1, n - 1, 2) if i != half - 1]
    rnear = lax.ppermute(cmo, "lane", pairs + [(j, i) for i, j in pairs])
    (hand,) = call(relay, [lane_mass], [VM])(redges)
    pairs = [(half - 2, half + 1), (n - 2, 1)]
    rhand = lax.ppermute(hand, "lane", pairs + [(j, i) for i, j in pairs])
    racross = swap_even(rhand, "lane")

    u, f, w, a4, v1, v2, v3, cl, token = call(
        prepare,
        [fine] * 7 + [own_coarse, sds(8, L)],
        [HBM, HBM, VM],
        [own_buf, own_buf, line, dma((2,))],
        flops=10**8,
    )(load, start, mass_in)

    ce, co = call(pack_corners, [corner, corner], [VM] * 3)(re, ro, token)
    rco, rce = swap_odd(co, "band"), swap_even(ce, "band")

    mext, mbe, mbo = call(
        functools.partial(mass_bands, n), [coarse, band_coarse, band_coarse], [VM] * 4
    )(cm, redges, rnear, racross)
    rmbo, rmbe = swap_odd(mbo, "band"), swap_even(mbe, "band")

    u, f, w, v1, v2, v3, cl = call(
        from_lanes,
        [fine] * 6 + [own_coarse],
        [VM] * 10,
        [pltpu.VMEM((N * DF, L), f32), pltpu.VMEM((N * DF, L), f32)],
        aliases={k: k for k in range(7)},
        flops=10**7,
    )(u, f, w, v1, v2, v3, cl, a4, re, ro)

    u, f, w, v1, v2, v3, cl, le, lo, rime, rimo = call(
        before,
        [fine] * 6 + [own_coarse, lane_coarse, lane_coarse, early, early],
        [VM] * 12,
        [pltpu.VMEM(corner.shape, f32), line],
        aliases={k: k for k in range(7)},
        flops=10**8,
    )(u, f, w, v1, v2, v3, cl, a4, rbe, rbo, rce, rco)
    rlo, rle = swap_odd(lo, "lane"), swap_even(le, "lane")
    rrimo, rrime = swap_odd(rimo, "band"), swap_even(rime, "band")
    lext, lbe, lbo = call(coarse_bands, [coarse, band_late, band_late], [VM] * 3)(cl, rle, rlo)
    rlbo, rlbe = swap_odd(lbo, "band"), swap_even(lbe, "band")
    v3, lext, wext, first = call(
        between,
        [fine, coarse, coarse, coarse],
        [VM] * 9,
        [coarse_buf],
        aliases={0: 0, 1: 1},
        flops=10**7,
    )(v3, lext, mext, rmbe, rmbo, rle, rlo, rrime, rrimo)

    out, *_ = call(
        after,
        [own, coarse, coarse],
        [VM] * 8,
        [coarse_buf] + [pltpu.VMEM((N + 8, L), f32), fine_buf, fine_buf, own_buf, dma((PIECES,))],
        flops=10**8,
        aliases={4: 1, 5: 2},
        result=True,
    )(v3, f, w, wext, lext, first, rlbe, rlbo)
    return out


def solution(mesh):
    spec = P("band", "lane", None)

    return jax.shard_map(
        shards, mesh=mesh, in_specs=(spec, spec, spec), out_specs=spec, check_vma=False
    )
```

```python
import functools

import jax
import jax.numpy as jnp
from jax import lax
from jax.experimental import pallas as pl
from jax.experimental.pallas import tpu as pltpu
from jax.sharding import PartitionSpec as P


RATIO = 4
BEFORE = 3
AFTER = 2
INNER = 13

N = 64
C = N // RATIO
L = 128
DS = BEFORE + 1
DF = DS - 1
DEPTH = DS + 2 * DF
AT_LOAD, AT_MASS = N * DS, N * (DS + DF)
FINE = N * DEPTH
R0, C0 = DS, 12
R1, C1 = R0 + N, C0 + N
ROWS, COLS = R1 + DS, C1 + 12
FULL = ((C0 - 4, C0 + 20), (C0 + 20, C0 + 44), (C0 + 44, C0 + 68))
EDGES = ((C0 - 4, C0 + 4), (C1 - 4, C1 + 4))
H = INNER
CR0, CC0 = H, 20
CR, CCOLS = C + 2 * H, 56
WIDTHS = [C + 2 * (H + 1 - j) for j in range(1, H + 1)]
STARTS = [sum(WIDTHS[:k]) for k in range(H)]
BAND_COARSE = -(-sum(WIDTHS) // 8) * 8
BAND_OWN = C * H
BAND_RIM = N + 8
BAND_LATE = -(-H * (H + 1) // 8) * 8
REACHES = [(j, H + 1 - j, (j - 1) * (2 * H + 2) - (j - 1) * j) for j in range(1, H + 1)]
LANE_COARSE = C * H
PIECES = 16
FIT = 16 * 2**20

f32 = jnp.float32


def parity(axis):
    return lax.rem(lax.axis_index(axis), 2) == 0


def either(test, one, other):
    @pl.when(test)
    def _():
        one()

    @pl.when(jnp.logical_not(test))
    def _():
        other()


def sds(*shape):
    return jax.ShapeDtypeStruct(shape, f32)


VM = pl.BlockSpec(memory_space=pltpu.VMEM)
HBM = pl.BlockSpec(memory_space=pltpu.HBM)


def call(body, outs, ins, scratch=(), aliases=None, flops=10**6, result=False):
    return pl.pallas_call(
        body,
        out_shape=outs[:result] + [pltpu.VMEM(o.shape, o.dtype) for o in outs[result:]],
        in_specs=ins,
        out_specs=[HBM] * result + [VM] * (len(outs) - result),
        scratch_shapes=list(scratch),
        input_output_aliases=aliases or {},
        compiler_params=pltpu.CompilerParams(vmem_limit_bytes=FIT),
        cost_estimate=pl.CostEstimate(flops=flops, bytes_accessed=8 * 10**6, transcendentals=0),
    )


def loop(count, per, body):
    def turn(g, carry):
        for k in range(per):
            body(g * per + k)
        return carry

    lax.fori_loop(0, count // per, turn, 0)


def gather_columns(line, row):
    line[...] = row
    total = line[pl.ds(0, C, stride=RATIO), :]
    for k in range(1, RATIO):
        total = total + line[pl.ds(k, C, stride=RATIO), :]
    return total * (1.0 / RATIO)


def pack_fine(load, start, mass_hbm, m_even, m_odd, b_even, b_odd, mass, cm, edges, c_odd, side, line, sem_side, sem_mass, sem_band):
    whole = pltpu.make_async_copy(mass_hbm, mass, sem_mass.at[0])
    copies = []
    for k, src in enumerate((start, load)):
        for s, at in enumerate((0, N - 8)):
            copies.append(
                pltpu.make_async_copy(src.at[:, pl.ds(at, 8)], side.at[k, s], sem_side.at[k, s])
            )
    even = parity("band")
    bands = []
    for which, (dst, bottom) in enumerate(((b_even, even), (b_odd, jnp.logical_not(even)))):
        at = 0
        for k, (src, depth) in enumerate(((start, DS), (load, DF), (mass_hbm, DF))):
            first = jnp.where(bottom, N - depth, 0)
            bands.append(
                pltpu.make_async_copy(
                    src.at[pl.ds(first, depth)], dst.at[pl.ds(at, depth)], sem_band.at[which, k]
                )
            )
            at += depth
    for c in copies:
        c.start()
    whole.start()
    for c in bands:
        c.start()
    for c in copies:
        c.wait()

    def pack(right, left):
        def group(g, carry):
            for k, (depth, field) in enumerate(((DS, 0), (DF, AT_LOAD))):
                base = pl.multiple_of(g * (8 * depth), 8)
                for r in range(8):
                    at = field + base + r * depth
                    right[pl.ds(at, depth), :] = side[k, 1, g * 8 + r, 8 - depth :, :]
                    left[pl.ds(at, depth), :] = side[k, 0, g * 8 + r, :depth, :]
            return carry

        lax.fori_loop(0, N // 8, group, 0)

    lane_even = parity("lane")
    either(lane_even, lambda: pack(m_even, m_odd), lambda: pack(m_odd, m_even))
    whole.wait()

    def pack_mass(right, left):
        def group(g, carry):
            base = pl.multiple_of(g * (8 * DF), 8)
            for half in range(2):
                total = None
                for k in range(RATIO):
                    r = half * RATIO + k
                    at = AT_MASS + base + r * DF
                    row = mass[g * 8 + r]
                    total = row if total is None else total + row
                    right[pl.ds(at, DF), :] = row[N - DF :, :]
                    left[pl.ds(at, DF), :] = row[:DF, :]
                cm[2 * g + half] = gather_columns(line.at[half], total)
            return carry

        lax.fori_loop(0, N // 8, group, 0)

    either(
        lane_even,
        lambda: pack_mass(m_even, m_odd),
        lambda: pack_mass(m_odd, m_even),
    )
    for i in range(C):
        row = cm[i]
        edges[i * H : (i + 1) * H, :] = row[:H, :]
        edges[LANE_COARSE + i * H : LANE_COARSE + (i + 1) * H, :] = row[C - H :, :]

    def odd_side(first):
        c_odd[...] = edges[first : first + LANE_COARSE, :]

    either(lane_even, lambda: odd_side(0), lambda: odd_side(LANE_COARSE))
    for c in bands:
        c.wait()


def pack_corners(m_even, m_odd, token, c_even, c_odd):
    del token

    def fill(left, right):
        def put(dst, bottom):
            at = 0
            for src in (left, right):
                for field, depth in ((0, DS), (AT_LOAD, DF), (AT_MASS, DF)):
                    lo, size = field + (N - DF) * depth * bottom, DF * depth
                    dst[at : at + size, :] = src[lo : lo + size, :]
                    at += size

        either(
            parity("band"),
            lambda: (put(c_even, 1), put(c_odd, 0)),
            lambda: (put(c_even, 0), put(c_odd, 1)),
        )

    either(parity("lane"), lambda: fill(m_odd, m_even), lambda: fill(m_even, m_odd))


def pack_coarse_lanes(own, right, left, at):
    for i in range(C):
        lo = at + i * H
        row = own[i]
        right[lo : lo + H, :] = row[C - H :, :]
        left[lo : lo + H, :] = row[:H, :]


def place_coarse_lanes(ext, left, right, at_left=0, at_right=0):
    for i in range(C):
        ext[CR0 + i, CC0 - H : CC0, :] = left[at_left + i * H : at_left + (i + 1) * H, :]
        ext[CR0 + i, CC0 + C : CC0 + C + H, :] = right[at_right + i * H : at_right + (i + 1) * H, :]


def pack_coarse_bands(ext, down, up):
    for j in range(1, H + 1):
        reach, at, wide = H + 1 - j, STARTS[j - 1], WIDTHS[j - 1]
        cols = slice(CC0 - reach, CC0 + C + reach)
        down[at : at + wide, :] = ext[CR0 + C - j, cols, :]
        up[at : at + wide, :] = ext[CR0 + j - 1, cols, :]
    for dst in (down, up):
        dst[sum(WIDTHS) : BAND_COARSE, :] = jnp.zeros((BAND_COARSE - sum(WIDTHS), L), f32)


def place_coarse_bands(ext, above, below):
    for j in range(1, H + 1):
        reach, at, wide = H + 1 - j, STARTS[j - 1], WIDTHS[j - 1]
        cols = slice(CC0 - reach, CC0 + C + reach)
        ext[CR0 - j, cols, :] = above[at : at + wide, :]
        ext[CR0 + C + j - 1, cols, :] = below[at : at + wide, :]


def pack_late(ext, down, up):
    for j, reach, at in REACHES:
        for dst, row in ((down, CR0 + C - j), (up, CR0 + j - 1)):
            dst[at : at + reach, :] = ext[row, CC0 - reach : CC0, :]
            dst[at + reach : at + 2 * reach, :] = ext[row, CC0 + C : CC0 + C + reach, :]
    for dst in (down, up):
        dst[H * (H + 1) :, :] = jnp.zeros((BAND_LATE - H * (H + 1), L), f32)


def place_late(ext, a, wext, above, below):
    for j, reach, at in REACHES:
        for msg, row in ((above, CR0 - j), (below, CR0 + C + j - 1)):
            for lo, first in ((at, CC0 - reach), (at + reach, CC0 + C)):
                cols = slice(first, first + reach)
                values = msg[lo : lo + reach, :]
                ext[row, cols, :] = values
                a[row, cols, :] = wext[row, cols, :] * values


def weight(mass):
    return 0.8 / (4.0 + mass)


def sweep_rows(src, dst, w, f, first, last, segments, per=4):
    def some(r, count):
        for lo, hi in segments:
            line = [src[r - 1 + k, lo:hi, :] for k in range(count + 2)]
            for k in range(count):
                q = r + k
                around = (line[k] + line[k + 2]) + (
                    src[q, lo - 1 : hi - 1, :] + src[q, lo + 1 : hi + 1, :]
                )
                dst[q, lo:hi, :] = 0.2 * line[k + 1] + w[q, lo:hi, :] * (f[q, lo:hi, :] + around)

    whole = (last - first) // per
    if whole > 1:

        def group(g, carry):
            some(first + g * per, per)
            return carry

        lax.fori_loop(0, whole, group, 0)
        first = first + whole * per
    for r in range(first, last, per):
        some(r, min(per, last - r))


def defect_sum(v, f, a4, first, lo, hi):
    total = None
    line = [v[first - 1 + k, lo:hi, :] for k in range(RATIO + 2)]
    for k in range(RATIO):
        q = first + k
        around = (line[k] + line[k + 2]) + (v[q, lo - 1 : hi - 1, :] + v[q, lo + 1 : hi + 1, :])
        one = (f[q, lo:hi, :] + around) - a4[q, lo:hi, :] * line[k + 1]
        total = one if total is None else total + one
    return total


def prepare(load, start, mass, u, f, w, a4, v1, v2, v3, cl, token, line):
    def own(r):
        a = 4.0 + mass[r]
        a4[R0 + r, C0:C1, :] = a
        w[R0 + r, C0:C1, :] = 0.8 / a
        f[R0 + r, C0:C1, :] = load[r]
        u[R0 + r, C0:C1, :] = start[r]

    loop(N, 2, own)
    sweep_rows(u, v1, w, f, R0 + 1, R1 - 1, FULL)
    sweep_rows(v1, v2, w, f, R0 + 2, R1 - 2, FULL)
    sweep_rows(v2, v3, w, f, R0 + 3, R1 - 3, FULL)

    def block(i, carry):
        cl[i] = gather_columns(line, defect_sum(v3, f, a4, R0 + RATIO * i, C0, C1))
        return carry

    lax.fori_loop(1, C - 1, block, 0)
    token[...] = jnp.zeros((8, L), f32)


def from_lanes(u_in, f_in, w_in, v1_in, v2_in, v3_in, cl_in, a4, re, ro, u, f, w, v1, v2, v3, cl, wl, wr):
    del u_in, f_in, w_in, v1_in, v2_in, v3_in, cl_in

    def lanes(left, right):
        for msg, out in ((left, wl), (right, wr)):
            out[...] = weight(msg[AT_MASS:FINE, :])
        for msg, out, cs, cf in ((left, wl, C0 - DS, C0 - DF), (right, wr, C1, C1)):

            def group(g, carry):
                s0, f0 = pl.multiple_of(g * (8 * DS), 8), pl.multiple_of(g * (8 * DF), 8)
                for r in range(8):
                    row = R0 + g * 8 + r
                    u[row, cs : cs + DS, :] = msg[pl.ds(s0 + r * DS, DS), :]
                    f[row, cf : cf + DF, :] = msg[pl.ds(AT_LOAD + f0 + r * DF, DF), :]
                    w[row, cf : cf + DF, :] = out[pl.ds(f0 + r * DF, DF), :]
                return carry

            lax.fori_loop(0, N // 8, group, 0)

    either(parity("lane"), lambda: lanes(ro, re), lambda: lanes(re, ro))
    for src, dst, k in ((u, v1, 1), (v1, v2, 2), (v2, v3, 3)):
        sweep_rows(src, dst, w, f, R0 + k, R1 - k, EDGES)

    def rims(i, carry):
        row = R0 + RATIO * i
        left = defect_sum(v3, f, a4, row, C0 - 4, C0 + 4)
        right = defect_sum(v3, f, a4, row, C1 - 4, C1 + 4)
        cl[i, 0:1, :] = jnp.sum(left[4:8, :], axis=0, keepdims=True) * (1.0 / RATIO)
        cl[i, C - 1 : C, :] = jnp.sum(right[0:4, :], axis=0, keepdims=True) * (1.0 / RATIO)
        return carry

    lax.fori_loop(1, C - 1, rims, 0)


def before(u_in, f_in, w_in, v1_in, v2_in, v3_in, cl_in, a4, be, bo, ce, co, u, f, w, v1, v2, v3, cl, l_even, l_odd, rim_even, rim_odd, wc, line):
    del u_in, f_in, w_in, v1_in, v2_in, v3_in, cl_in

    lane_even, band_even = parity("lane"), parity("band")

    def bands(above, below, above_c, below_c):
        own = slice(C0, C1)
        for msg, row in ((above, R0), (below, R1)):
            first = row - DS if row == R0 else row
            for k in range(DS):
                u[first + k, own, :] = msg[k]
            first = row - DF if row == R0 else row
            for k in range(DF):
                f[first + k, own, :] = msg[DS + k]
                w[first + k, own, :] = weight(msg[DS + DF + k])
        for msg, first in ((above_c, R0 - DF), (below_c, R1)):
            half = DF * DEPTH
            wc[...] = weight(msg[...])
            for at, cs, cf in ((0, C0 - DS, C0 - DF), (half, C1, C1)):
                for k in range(DF):
                    row = first + k
                    s0, l0, m0 = at + k * DS, at + DF * DS + k * DF, at + DF * (DS + DF) + k * DF
                    u[row, cs : cs + DS, :] = msg[s0 : s0 + DS, :]
                    f[row, cf : cf + DF, :] = msg[l0 : l0 + DF, :]
                    w[row, cf : cf + DF, :] = wc[m0 : m0 + DF, :]

    either(band_even, lambda: bands(bo, be, co, ce), lambda: bands(be, bo, ce, co))

    for src, dst, k in ((u, v1, 1), (v1, v2, 2), (v2, v3, 3)):
        reach = BEFORE + 1 - k
        sweep_rows(src, dst, w, f, R0 - reach, R0 + k, FULL)
        sweep_rows(src, dst, w, f, R1 - k, R1 + reach, FULL)

    for i in (0, C - 1):
        cl[i] = gather_columns(line, defect_sum(v3, f, a4, R0 + RATIO * i, C0, C1))

    def out_lanes(right, left):
        pack_coarse_lanes(cl, right, left, 0)

        def group(g, carry):
            base = pl.multiple_of(g * 8, 8)
            for r in range(8):
                row = R0 + g * 8 + r
                right[pl.ds(LANE_COARSE + base + r, 1), :] = v3[row, C1 - 2 : C1 - 1, :]
                left[pl.ds(LANE_COARSE + base + r, 1), :] = v3[row, C0 + 1 : C0 + 2, :]
            return carry

        lax.fori_loop(0, N // 8, group, 0)

    either(lane_even, lambda: out_lanes(l_even, l_odd), lambda: out_lanes(l_odd, l_even))

    def out_bands(down, up):
        for j in range(1, H + 1):
            down[(j - 1) * C : j * C, :] = cl[C - j]
            up[(j - 1) * C : j * C, :] = cl[j - 1]
        for dst, rim, edge in ((down, R1 - 2, R1 - 1), (up, R0 + 1, R0)):
            at = BAND_OWN
            dst[at : at + N, :] = v3[rim, C0:C1, :]
            dst[at + N : at + N + 8, :] = jnp.zeros((8, L), f32)
            dst[at + N : at + N + 1, :] = v3[edge, C0 - 1 : C0, :]
            dst[at + N + 1 : at + N + 2, :] = v3[edge, C1 : C1 + 1, :]

    either(band_even, lambda: out_bands(rim_even, rim_odd), lambda: out_bands(rim_odd, rim_even))


def relay(edges, out):
    def put(first):
        out[...] = edges[first : first + LANE_COARSE, :]

    either(parity("lane"), lambda: put(LANE_COARSE), lambda: put(0))


def far(lane, lanes):
    at = lax.rem(lane, lanes // 2)
    return (at == 0) | (at == lanes // 2 - 1)


def mass_bands(lanes, cm, edges, near, across, mext, b_even, b_odd):
    for i in range(C):
        mext[CR0 + i, CC0 : CC0 + C, :] = cm[i]

    def place(odd):
        either(
            parity("lane"),
            lambda: place_coarse_lanes(mext, odd, edges),
            lambda: place_coarse_lanes(mext, edges, odd, LANE_COARSE),
        )

    either(far(lax.axis_index("lane"), lanes), lambda: place(across), lambda: place(near))
    either(
        parity("band"),
        lambda: pack_coarse_bands(mext, b_even, b_odd),
        lambda: pack_coarse_bands(mext, b_odd, b_even),
    )


def coarse_bands(cl, re, ro, lext, b_even, b_odd):
    for i in range(C):
        lext[CR0 + i, CC0 : CC0 + C, :] = cl[i]
    either(
        parity("lane"),
        lambda: place_coarse_lanes(lext, ro, re),
        lambda: place_coarse_lanes(lext, re, ro),
    )
    either(
        parity("band"),
        lambda: pack_late(lext, b_even, b_odd),
        lambda: pack_late(lext, b_odd, b_even),
    )


def between(v_in, lext_in, mext, mbe, mbo, le, lo, rbe, rbo, v, lext, wext, a, ext):
    del v_in, lext_in

    def lanes(left, right):
        def group(g, carry):
            base = pl.multiple_of(g * 8, 8)
            for r in range(8):
                row = R0 + g * 8 + r
                v[row, C0 - 2 : C0 - 1, :] = left[pl.ds(LANE_COARSE + base + r, 1), :]
                v[row, C1 + 1 : C1 + 2, :] = right[pl.ds(LANE_COARSE + base + r, 1), :]
            return carry

        lax.fori_loop(0, N // 8, group, 0)

    either(parity("lane"), lambda: lanes(lo, le), lambda: lanes(le, lo))
    span = slice(CC0 - H, CC0 + C + H)
    for i in range(C):
        ext[CR0 + i, span, :] = mext[CR0 + i, span, :]

    def own(above, below):
        for j in range(1, H + 1):
            lext[CR0 - j, CC0 : CC0 + C, :] = above[(j - 1) * C : j * C, :]
            lext[CR0 + C + j - 1, CC0 : CC0 + C, :] = below[(j - 1) * C : j * C, :]
        for msg, rim, edge in ((above, R0 - 2, R0 - 1), (below, R1 + 1, R1)):
            at = BAND_OWN
            v[rim, C0:C1, :] = msg[at : at + N, :]
            v[edge, C0 - 1 : C0, :] = msg[at + N : at + N + 1, :]
            v[edge, C1 : C1 + 1, :] = msg[at + N + 1 : at + N + 2, :]

    either(parity("band"), lambda: own(rbo, rbe), lambda: own(rbe, rbo))

    def bands(above, below):
        place_coarse_bands(ext, above, below)

    either(parity("band"), lambda: bands(mbo, mbe), lambda: bands(mbe, mbo))

    def weights(r):
        wc = weight(ext[r])
        wext[r] = wc
        a[r] = wc * lext[r]

    loop(CR, 2, weights)


def after(v, f, w, wext, lext_in, a_in, lbe, lbo, result, lext, a, b, wide, t, s, out, sems):
    del lext_in, a_in
    either(
        parity("band"),
        lambda: place_late(lext, a, wext, lbo, lbe),
        lambda: place_late(lext, a, wext, lbe, lbo),
    )

    src, dst = a, b
    for k in range(1, INNER):
        first = CC0 - H + k
        wide_by = -(-(CR - 2 * k) // 8) * 8
        segments = ((first, first + 16), (first + 16, first + wide_by)) if wide_by > 24 else ((first, first + 24),)
        sweep_rows(src, dst, wext, lext, k, CR - k, segments)
        src, dst = dst, src

    def correct(i):
        row = src[CR0 + i, CC0 - 1 : CC0 + C + 1, :]
        for k in range(RATIO):
            wide[pl.ds(k, C + 2, stride=RATIO), :] = row
        for k in range(RATIO):
            q = i * RATIO + k
            if -AFTER <= q < N + AFTER:
                t[R0 + q, C0 - 4 : C1 + 4, :] = v[R0 + q, C0 - 4 : C1 + 4, :] + wide[...]

    def last(r, carry):
        for lo, hi in ((0, 32), (32, 64)):
            line = [s[R0 + 4 * r - 1 + k, C0 + lo : C0 + hi, :] for k in range(6)]
            for k in range(4):
                q = R0 + 4 * r + k
                around = (line[k] + line[k + 2]) + (
                    s[q, C0 + lo - 1 : C0 + hi - 1, :] + s[q, C0 + lo + 1 : C0 + hi + 1, :]
                )
                out[4 * r + k, lo:hi, :] = 0.2 * line[k + 1] + w[q, C0 + lo : C0 + hi, :] * (
                    f[q, C0 + lo : C0 + hi, :] + around
                )
        return carry

    copies = []
    rows = N // PIECES
    corrected, swept = -1, R0 - 1
    for piece in range(PIECES):
        end = (piece + 1) * rows
        upto = min(C, (end + 1) // RATIO)
        for i in range(corrected, upto + 1):
            correct(i)
        corrected = upto + 1
        sweep_rows(t, s, w, f, swept, R0 + end + 1, FULL)
        swept = R0 + end + 1
        lax.fori_loop(piece * rows // 4, end // 4, last, 0)
        span = pl.ds(piece * rows, rows)
        copies.append(pltpu.make_async_copy(out.at[span], result.at[span], sems.at[piece]))
        copies[-1].start()
    for c in copies:
        c.wait()


def swap_even(x, axis):
    n = lax.axis_size(axis)
    return lax.ppermute(x, axis, [(i, i ^ 1) for i in range(n)])


def swap_odd(x, axis):
    n = lax.axis_size(axis)
    return lax.ppermute(x, axis, [(i, (i + 1) % n if i % 2 else (i - 1) % n) for i in range(n)])


def shards(load, start, mass):
    raw = (load, start)
    load, start, mass = (pltpu.with_memory_space_constraint(x, pltpu.HBM) for x in (load, start, mass))
    dma = pltpu.SemaphoreType.DMA
    own, fine = sds(N, N, L), sds(ROWS, COLS, L)
    corner = sds(2 * DF * DEPTH, L)
    lane_msg, band_msg = sds(FINE, L), sds(DEPTH, N, L)
    early, lane_mass = sds(BAND_OWN + BAND_RIM, L), sds(LANE_COARSE, L)
    lane_coarse, band_coarse = sds(LANE_COARSE + N, L), sds(BAND_COARSE, L)
    band_late = sds(BAND_LATE, L)
    coarse, own_coarse = sds(CR, CCOLS, L), sds(C, C, L)
    coarse_buf, fine_buf = pltpu.VMEM((CR, CCOLS, L), f32), pltpu.VMEM((ROWS, COLS, L), f32)
    own_buf, line = pltpu.VMEM((N, N, L), f32), pltpu.VMEM((N, L), f32)

    me, mo, be, bo, mass_in, cm, edges, cmo = call(
        pack_fine,
        [lane_msg, lane_msg, band_msg, band_msg, own, own_coarse, sds(2 * LANE_COARSE, L), lane_mass],
        [HBM] * 3,
        [pltpu.VMEM((2, 2, N, 8, L), f32), pltpu.VMEM((2, N, L), f32), dma((2, 2)), dma((1,)), dma((2, 3))],
    )(load, start, mass)
    rbo, rbe = swap_odd(bo, "band"), swap_even(be, "band")
    ro, re = swap_odd(mo, "lane"), swap_even(me, "lane")

    n = lax.axis_size("lane")
    half = n // 2
    redges = swap_even(edges, "lane")
    pairs = [(i, i + 1) for i in range(1, n - 1, 2) if i != half - 1]
    rnear = lax.ppermute(cmo, "lane", pairs + [(j, i) for i, j in pairs])
    (hand,) = call(relay, [lane_mass], [VM])(redges)
    pairs = [(half - 2, half + 1), (n - 2, 1)]
    rhand = lax.ppermute(hand, "lane", pairs + [(j, i) for i, j in pairs])
    racross = swap_even(rhand, "lane")

    *raw, mass_in = lax.optimization_barrier((*raw, mass_in))
    load_in, start_in = (pltpu.with_memory_space_constraint(x, pltpu.VMEM) for x in raw)
    u, f, w, a4, v1, v2, v3, cl, token = call(
        prepare, [fine] * 7 + [own_coarse, sds(8, L)], [VM] * 3, [line], flops=10**8
    )(load_in, start_in, mass_in)

    ce, co = call(pack_corners, [corner, corner], [VM] * 3)(re, ro, token)
    rco, rce = swap_odd(co, "band"), swap_even(ce, "band")

    mext, mbe, mbo = call(
        functools.partial(mass_bands, n), [coarse, band_coarse, band_coarse], [VM] * 4
    )(cm, redges, rnear, racross)
    rmbo, rmbe = swap_odd(mbo, "band"), swap_even(mbe, "band")

    u, f, w, v1, v2, v3, cl = call(
        from_lanes,
        [fine] * 6 + [own_coarse],
        [VM] * 10,
        [pltpu.VMEM((N * DF, L), f32), pltpu.VMEM((N * DF, L), f32)],
        aliases={k: k for k in range(7)},
        flops=10**7,
    )(u, f, w, v1, v2, v3, cl, a4, re, ro)

    u, f, w, v1, v2, v3, cl, le, lo, rime, rimo = call(
        before,
        [fine] * 6 + [own_coarse, lane_coarse, lane_coarse, early, early],
        [VM] * 12,
        [pltpu.VMEM(corner.shape, f32), line],
        aliases={k: k for k in range(7)},
        flops=10**8,
    )(u, f, w, v1, v2, v3, cl, a4, rbe, rbo, rce, rco)
    rlo, rle = swap_odd(lo, "lane"), swap_even(le, "lane")
    rrimo, rrime = swap_odd(rimo, "band"), swap_even(rime, "band")
    lext, lbe, lbo = call(coarse_bands, [coarse, band_late, band_late], [VM] * 3)(cl, rle, rlo)
    rlbo, rlbe = swap_odd(lbo, "band"), swap_even(lbe, "band")
    v3, lext, wext, first = call(
        between,
        [fine, coarse, coarse, coarse],
        [VM] * 9,
        [coarse_buf],
        aliases={0: 0, 1: 1},
        flops=10**7,
    )(v3, lext, mext, rmbe, rmbo, rle, rlo, rrime, rrimo)

    out, *_ = call(
        after,
        [own, coarse, coarse],
        [VM] * 8,
        [coarse_buf] + [pltpu.VMEM((N + 8, L), f32), fine_buf, fine_buf, own_buf, dma((PIECES,))],
        flops=10**8,
        aliases={4: 1, 5: 2},
        result=True,
    )(v3, f, w, wext, lext, first, rlbe, rlbo)
    return out


def solution(mesh):
    spec = P("band", "lane", None)

    return jax.shard_map(
        shards, mesh=mesh, in_specs=(spec, spec, spec), out_specs=spec, check_vma=False
    )
```
